16 devices in a mesh: dp: 2 (over y, z), tp: 8 (over x, core).
Axes of the slice: x: 4, y: 2, z: 1, core: 2. Of those that a mesh axis runs over, the one named last changes fastest.
The devices are a block of a 4x4x8 slice.
Arguments:
- x: bfloat16 [5632, 3072], P(('dp', 'tp')), parts along dimension 0
- dy: bfloat16 [5632, 3072], P(('dp', 'tp')), parts along dimension 0
- pre: bfloat16 [5632, 9216], P('dp', 'tp'), parts along dimension 0
- w_in: bfloat16 [3072, 9216], P(None, 'tp')
- w_down: bfloat16 [9216, 3072], P('tp')
Outputs:
- output 1: bfloat16 [5632, 3072], P(('dp', 'tp')), parts along dimension 0
- output 2: bfloat16 [6144, 9216], P('dp', 'tp'), parts along dimension 0
- output 3: bfloat16 [18432, 3072], P(('dp', 'tp')), parts along dimension 0
There are 2 independent parts. The reference program is written for one: setup_inputs(seed, part) draws one part's arguments, and reference() takes and returns one part's arrays. A program takes and returns all parts, laid end to end along the dimension named above; an argument that names none is the same for every part.
All inputs are finite; a program needn't handle non-finite values.
Results may differ from the reference program's by a relative error of at most 0.012.
Values are sent between devices in bfloat16 or wider.
A program may use at most 768 MiB of HBM per device.

```python
import jax
import jax.numpy as jnp

ROWS = 2816
D = 3072
FF = 9216


def act(pre):
    return jnp.square(jax.nn.relu(pre))


def setup_inputs(seed: int = 0, part: int = 0) -> dict:
    kx, ky, ka, ki, kd = jax.random.split(jax.random.key(seed), 5)
    kx, ky, ka = (jax.random.fold_in(k, part) for k in (kx, ky, ka))
    drawn = {
        "x": jax.random.normal(kx, (ROWS, D), jnp.float32),
        "dy": jax.random.normal(ky, (ROWS, D), jnp.float32),
        "pre": jax.random.normal(ka, (ROWS, FF), jnp.float32),
        "w_in": jax.random.normal(ki, (D, FF), jnp.float32) * D**-0.5,
        "w_down": jax.random.normal(kd, (FF, D), jnp.float32) * FF**-0.5,
    }
    return {k: v.astype(jnp.bfloat16) for k, v in drawn.items()}


def reference(x, dy, pre, w_in, w_down):
    hidden, back = jax.vjp(act, pre.astype(jnp.float32))
    d_hidden = jnp.dot(dy, w_down.T, preferred_element_type=jnp.float32)
    d_pre = back(d_hidden)[0].astype(jnp.bfloat16)
    dx = jnp.dot(d_pre, w_in.T, preferred_element_type=jnp.float32)
    dw_in = jnp.dot(x.T, d_pre, preferred_element_type=jnp.float32)
    dw_down = jnp.dot(hidden.astype(jnp.bfloat16).T, dy, preferred_element_type=jnp.float32)
    return tuple(g.astype(jnp.bfloat16) for g in (dx, dw_in, dw_down))
```

```python
import functools

import jax
import jax.numpy as jnp
from jax import lax
from jax.experimental import pallas as pl
from jax.experimental.pallas import tpu as pltpu
from jax.sharding import PartitionSpec as P

CORES = 2
F32, BF16 = jnp.float32, jnp.bfloat16
NT = (((1,), (1,)), ((), ()))
TN = (((0,), (0,)), ((), ()))

(R0, R1, L0, L1, OWN, FR, FL, PL0, PL1, PR0, PR1, PO0, PO1) = range(13)
COPIES = 13


def gather_kernel(
    chips, x, dy, pre, w_in, w_down,
    xg, dyg, d_pre, s_own, s_left0, s_left1, s_right0, s_right1, s_far,
    wd_v, wi_v, wp_v, dy_v, pre_v, mine_v, other_v, got_v, acc_v, low_v,
    send_sem, recv_sem, got_send, got_recv, w_send, w_recv, load_sem, store_sem,
):
    rows, depth = dy.shape
    half = rows // 2
    cols = w_down.shape[0]
    me = lax.axis_index("tp")
    chip, core = me // CORES, lax.rem(me, CORES)
    left = lax.rem(chip + chips - 1, chips)
    right = lax.rem(chip + 1, chips)
    far = lax.rem(chip + 2, chips)

    def device(c, k):
        return {"tp": c * CORES + k}

    to_right, to_left, to_partner = device(right, core), device(left, core), device(chip, 1 - core)

    def block(ref, c, k, h=None):
        start = (c * CORES + k) * rows
        if h is None:
            return ref.at[pl.ds(pl.multiple_of(start, 16), rows)]
        return ref.at[pl.ds(pl.multiple_of(start + h * half, 16), half)]

    class Gather:
        def __init__(self, which, src, dst):
            self.which, self.src, self.dst = which, src, dst

        def own(self, h):
            return self.src.at[pl.ds(h * half, half)]

        def copy(self, n, src, dst, target):
            return pltpu.make_async_remote_copy(
                src_ref=src, dst_ref=dst, send_sem=send_sem.at[self.which, n], recv_sem=recv_sem.at[self.which, n],
                device_id=target, device_id_type=pl.DeviceIdType.MESH,
            )

        def out(self, n):
            d = self.dst
            if n in (R0, R1):
                h = n - R0
                return self.copy(n, self.own(h), block(d, chip, core, h), to_right)
            if n in (L0, L1):
                h = n - L0
                return self.copy(n, self.own(h), block(d, chip, core, h), to_left)
            if n == OWN:
                return self.copy(n, self.src, block(d, chip, core), to_partner)
            if n == FR:
                return self.copy(n, block(d, left, core, 0), block(d, left, core, 0), to_right)
            if n == FL:
                return self.copy(n, block(d, right, core, 1), block(d, right, core, 1), to_left)
            c, h = {PL0: (left, 0), PL1: (left, 1), PR0: (right, 0), PR1: (right, 1), PO0: (far, 0), PO1: (far, 1)}[n]
            return self.copy(n, block(d, c, core, h), block(d, c, core, h), to_partner)

        def start(self, *names):
            for n in names:
                self.out(n).start()

        def arrived(self, *names):
            for n in names:
                if n == OWN:
                    dst = block(self.dst, chip, 1 - core)
                else:
                    c, k, h = {
                        R0: (left, core, 0), R1: (left, core, 1), L0: (right, core, 0), L1: (right, core, 1),
                        FR: (far, core, 0), FL: (far, core, 1),
                        PL0: (left, 1 - core, 0), PL1: (left, 1 - core, 1), PR0: (right, 1 - core, 0),
                        PR1: (right, 1 - core, 1), PO0: (far, 1 - core, 0), PO1: (far, 1 - core, 1),
                    }[n]
                    dst = block(self.dst, c, k, h)
                self.copy(n, dst, dst, to_partner).wait_recv()

        def sent(self):
            for n in range(COPIES):
                self.out(n).wait_send()

    gy, gx = Gather(0, dy, dyg), Gather(1, x, xg)

    barrier = pltpu.get_barrier_semaphore()
    for target in (to_right, to_left, to_partner):
        pl.semaphore_signal(barrier, inc=1, device_id=target, device_id_type=pl.DeviceIdType.MESH)
    load_wd = pltpu.make_async_copy(w_down, wd_v, load_sem.at[0])
    load_dy = pltpu.make_async_copy(dy, dy_v, load_sem.at[1])
    load_x = pltpu.make_async_copy(x, low_v, load_sem.at[2])
    load_wi = pltpu.make_async_copy(w_in, wi_v, load_sem.at[3])
    load_dy.start()
    load_wd.start()
    pl.semaphore_wait(barrier, 3)

    gy.start(R0, L1, OWN, R1, L0)
    load_x.start()
    load_wi.start()
    give_w = pltpu.make_async_remote_copy(
        src_ref=w_in, dst_ref=wp_v, send_sem=w_send, recv_sem=w_recv,
        device_id=to_partner, device_id_type=pl.DeviceIdType.MESH,
    )
    give_w.start()

    load_dy.wait()
    keep_dy = pltpu.make_async_copy(dy_v, block(dyg, chip, core), store_sem.at[0])
    keep_dy.start()
    load_x.wait()
    keep_x = pltpu.make_async_copy(low_v, block(xg, chip, core), store_sem.at[1])
    keep_x.start()
    load_wd.wait()
    load_wi.wait()

    def chip_of(stage):
        return lax.rem(chip + jnp.where(stage == 0, 0, jnp.where(stage == 1, chips - 1, stage - 1)), chips)

    def hidden_grad(stage, k, out_v):
        c = chip_of(stage)
        load_pre = pltpu.make_async_copy(block(pre, c, k), pre_v, load_sem.at[0])
        load_pre.start()
        load = pltpu.make_async_copy(block(dyg, c, k), dy_v, load_sem.at[1])
        load.start()
        load.wait()
        load_pre.wait()
        tile = 384

        @pl.loop(0, cols // tile)
        def _(t):
            span = pl.ds(pl.multiple_of(t * tile, tile), tile)
            grad = lax.dot_general(dy_v[...], wd_v[span, :], NT, preferred_element_type=F32)
            p = pre_v[:, span].astype(F32)
            out_v[:, span] = jnp.where(p > 0, grad * (2.0 * p), 0.0).astype(BF16)

        keep = pltpu.make_async_copy(out_v, block(d_pre, c, k), store_sem.at[2])
        keep.start()
        return keep

    def swap(stage):
        return pltpu.make_async_remote_copy(
            src_ref=other_v, dst_ref=got_v.at[stage], send_sem=got_send, recv_sem=got_recv.at[stage],
            device_id=to_partner, device_id_type=pl.DeviceIdType.MESH,
        )

    keep_dy.wait()
    keep_x.wait()

    @pl.loop(0, chips)
    def _(stage):
        @pl.when(stage == 1)
        def _():
            gy.arrived(R0, L1)
            gy.start(FR, FL, PL0, PR1)
            gx.start(R0, L1, R1, L0, OWN)
            gy.arrived(R1, L0)
            gy.start(PL1, PR0)

        @pl.when(stage == 3)
        def _():
            gy.arrived(FR, FL)
            gy.start(PO0, PO1)

        hidden_grad(stage, core, mine_v).wait()

        @pl.when(stage == 0)
        def _():
            gy.arrived(OWN)

        @pl.when(stage == 1)
        def _():
            gy.arrived(PL0, PL1)

        @pl.when(stage == 2)
        def _():
            gy.arrived(PR0, PR1)

        @pl.when(stage == 3)
        def _():
            gy.arrived(PO0, PO1)

        keep = hidden_grad(stage, 1 - core, other_v)
        give = swap(stage)
        give.start()

        @pl.when(stage == 0)
        def _():
            give_w.wait()

        give.wait_recv()
        wide = 512

        @pl.loop(0, depth // wide)
        def _(t):
            span = pl.ds(pl.multiple_of(t * wide, wide), wide)
            term = lax.dot_general(mine_v[...], wi_v[span, :], NT, preferred_element_type=F32)
            term += lax.dot_general(got_v[stage], wp_v[span, :], NT, preferred_element_type=F32)
            acc_v[:, span] = term
            low_v[:, span] = term.astype(BF16)

        give.wait_send()
        keep.wait()
        top, bottom = pl.ds(0, half), pl.ds(half, half)

        def put(*pairs):
            copies = [pltpu.make_async_copy(s, d, store_sem.at[3 + i]) for i, (s, d) in enumerate(pairs)]
            for copy in copies:
                copy.start()
            for copy in copies:
                copy.wait()

        @pl.when(stage == 0)
        def _():
            put((acc_v, s_own))

        @pl.when(stage == 1)
        def _():
            put((low_v.at[top], s_left0), (acc_v.at[bottom], s_left1))

        @pl.when(stage == 2)
        def _():
            put((acc_v.at[top], s_right0), (low_v.at[bottom], s_right1))

        @pl.when(stage == 3)
        def _():
            put((low_v, s_far))

    gx.arrived(R0, L1)
    gx.start(FR, FL, PL0, PR1)
    gx.arrived(R1, L0)
    gx.start(PL1, PR0)
    gx.arrived(FR, FL)
    gx.start(PO0, PO1)
    gx.arrived(OWN, PL0, PL1, PR0, PR1, PO0, PO1)
    gy.sent()
    gx.sent()


def solution(mesh):
    n = mesh.shape["tp"]
    chips = n // CORES

    def gather(x, dy, pre, w_in, w_down):
        rows, depth = x.shape
        tokens, cols = pre.shape
        half = rows // 2
        anywhere = pl.BlockSpec(memory_space=pl.ANY)
        shape = jax.ShapeDtypeStruct
        return pl.pallas_call(
            functools.partial(gather_kernel, chips),
            name="gather",
            out_shape=(
                shape((tokens, depth), BF16),
                shape((tokens, depth), BF16),
                shape((tokens, cols), BF16),
                shape((rows, depth), F32),
                shape((half, depth), BF16),
                shape((half, depth), F32),
                shape((half, depth), F32),
                shape((half, depth), BF16),
                shape((rows, depth), BF16),
            ),
            in_specs=[anywhere] * 5,
            out_specs=(anywhere,) * 9,
            scratch_shapes=[
                pltpu.VMEM((cols, depth), BF16),
                pltpu.VMEM((depth, cols), BF16),
                pltpu.VMEM((depth, cols), BF16),
                pltpu.VMEM((rows, depth), BF16),
                pltpu.VMEM((rows, cols), BF16),
                pltpu.VMEM((rows, cols), BF16),
                pltpu.VMEM((rows, cols), BF16),
                pltpu.VMEM((chips, rows, cols), BF16),
                pltpu.VMEM((rows, depth), F32),
                pltpu.VMEM((rows, depth), BF16),
                pltpu.SemaphoreType.DMA((2, COPIES)),
                pltpu.SemaphoreType.DMA((2, COPIES)),
                pltpu.SemaphoreType.DMA,
                pltpu.SemaphoreType.DMA((chips,)),
                pltpu.SemaphoreType.DMA,
                pltpu.SemaphoreType.DMA,
                pltpu.SemaphoreType.DMA((4,)),
                pltpu.SemaphoreType.DMA((5,)),
            ],
            compiler_params=pltpu.CompilerParams(
                collective_id=0, has_side_effects=True, vmem_limit_bytes=64 * 1024 * 1024 - 65536
            ),
            cost_estimate=pl.CostEstimate(
                flops=4 * tokens * depth * cols, bytes_accessed=8 * tokens * depth, transcendentals=0
            ),
        )(x, dy, pre, w_in, w_down)

    def step(x, dy, pre, w_in, w_down):
        rows = x.shape[0]
        half = rows // 2
        clockwise = [(i, (i + CORES) % n) for i in range(n)]
        counter = [(i, (i - CORES) % n) for i in range(n)]
        xg, dyg, d_pre, s_own, s_left0, s_left1, s_right0, s_right1, s_far = gather(x, dy, pre, w_in, w_down)

        far0 = lax.ppermute(s_far[:half], "tp", clockwise)
        far1 = lax.ppermute(s_far[half:], "tp", counter)
        last1 = lax.ppermute(s_right1, "tp", clockwise)
        last0 = lax.ppermute(s_left0, "tp", counter)

        dw_in = lax.dot_general(xg, d_pre, TN, preferred_element_type=F32).astype(BF16)

        sum0 = lax.ppermute((s_right0 + far0.astype(F32)).astype(BF16), "tp", clockwise)
        sum1 = lax.ppermute((s_left1 + far1.astype(F32)).astype(BF16), "tp", counter)

        hidden = jnp.square(jax.nn.relu(pre.astype(F32))).astype(BF16)
        dw_down = lax.dot_general(hidden, dyg, TN, preferred_element_type=F32).astype(BF16)

        top = s_own[:half] + sum0.astype(F32) + last0.astype(F32)
        bottom = s_own[half:] + last1.astype(F32) + sum1.astype(F32)
        return jnp.concatenate([top, bottom]).astype(BF16), dw_in, dw_down

    tokens, columns, weight_rows = P(("dp", "tp"), None), P(None, "tp"), P("tp", None)
    return jax.shard_map(
        step,
        mesh=mesh,
        in_specs=(tokens, tokens, P("dp", "tp"), columns, weight_rows),
        out_specs=(tokens, P("dp", "tp"), P(("dp", "tp"), None)),
        check_vma=False,
    )
```

```python
import functools

import jax
import jax.numpy as jnp
from jax import lax
from jax.experimental import pallas as pl
from jax.experimental.pallas import tpu as pltpu
from jax.sharding import PartitionSpec as P

CORES = 2
F32, BF16 = jnp.float32, jnp.bfloat16
NT = (((1,), (1,)), ((), ()))
TN = (((0,), (0,)), ((), ()))

(R0, R1, L0, L1, OWN, FR, FL, PL0, PL1, PR0, PR1, PO0, PO1) = range(13)
COPIES = 13


def gather_kernel(
    chips, x, dy, pre, w_in, w_down,
    xg, dyg, d_pre, s_own, go_left, go_right, dw_down,
    wd_v, wi_v, wp_v, dy_v, pre_v, pair_v, got_v, acc_v, low_v, wait_v, far_v, dw_v,
    send_sem, recv_sem, got_send, got_recv, w_send, w_recv, far_send, far_recv, load_sem, store_sem,
):
    rows, depth = dy.shape
    half = rows // 2
    cols = w_down.shape[0]
    tile = 384
    first, top, bottom = pl.ds(0, rows), pl.ds(0, half), pl.ds(half, half)
    mine_v, other_v = pair_v.at[first], pair_v.at[pl.ds(rows, rows)]
    me = lax.axis_index("tp")
    chip, core = me // CORES, lax.rem(me, CORES)
    left = lax.rem(chip + chips - 1, chips)
    right = lax.rem(chip + 1, chips)
    far = lax.rem(chip + 2, chips)

    def device(c, k):
        return {"tp": c * CORES + k}

    to_right, to_left, to_partner = device(right, core), device(left, core), device(chip, 1 - core)

    def block(ref, c, k, h=None):
        start = (c * CORES + k) * rows
        if h is None:
            return ref.at[pl.ds(pl.multiple_of(start, 16), rows)]
        return ref.at[pl.ds(pl.multiple_of(start + h * half, 16), half)]

    class Gather:
        def __init__(self, which, src, dst):
            self.which, self.src, self.dst = which, src, dst

        def own(self, h):
            return self.src.at[pl.ds(h * half, half)]

        def copy(self, n, src, dst, target):
            return pltpu.make_async_remote_copy(
                src_ref=src, dst_ref=dst, send_sem=send_sem.at[self.which, n], recv_sem=recv_sem.at[self.which, n],
                device_id=target, device_id_type=pl.DeviceIdType.MESH,
            )

        def out(self, n):
            d = self.dst
            if n in (R0, R1):
                h = n - R0
                return self.copy(n, self.own(h), block(d, chip, core, h), to_right)
            if n in (L0, L1):
                h = n - L0
                return self.copy(n, self.own(h), block(d, chip, core, h), to_left)
            if n == OWN:
                return self.copy(n, self.src, block(d, chip, core), to_partner)
            if n == FR:
                return self.copy(n, block(d, left, core, 0), block(d, left, core, 0), to_right)
            if n == FL:
                return self.copy(n, block(d, right, core, 1), block(d, right, core, 1), to_left)
            c, h = {PL0: (left, 0), PL1: (left, 1), PR0: (right, 0), PR1: (right, 1), PO0: (far, 0), PO1: (far, 1)}[n]
            return self.copy(n, block(d, c, core, h), block(d, c, core, h), to_partner)

        def start(self, *names):
            for n in names:
                self.out(n).start()

        def arrived(self, *names):
            for n in names:
                if n == OWN:
                    dst = block(self.dst, chip, 1 - core)
                else:
                    c, k, h = {
                        R0: (left, core, 0), R1: (left, core, 1), L0: (right, core, 0), L1: (right, core, 1),
                        FR: (far, core, 0), FL: (far, core, 1),
                        PL0: (left, 1 - core, 0), PL1: (left, 1 - core, 1), PR0: (right, 1 - core, 0),
                        PR1: (right, 1 - core, 1), PO0: (far, 1 - core, 0), PO1: (far, 1 - core, 1),
                    }[n]
                    dst = block(self.dst, c, k, h)
                self.copy(n, dst, dst, to_partner).wait_recv()

        def sent(self):
            for n in range(COPIES):
                self.out(n).wait_send()

    gy, gx = Gather(0, dy, dyg), Gather(1, x, xg)

    barrier = pltpu.get_barrier_semaphore()
    for target in (to_right, to_left, to_partner):
        pl.semaphore_signal(barrier, inc=1, device_id=target, device_id_type=pl.DeviceIdType.MESH)
    load_wd = pltpu.make_async_copy(w_down, wd_v, load_sem.at[0])
    load_dy = pltpu.make_async_copy(dy, dy_v.at[first], load_sem.at[1])
    load_x = pltpu.make_async_copy(x, low_v, load_sem.at[2])
    load_wi = pltpu.make_async_copy(w_in, wi_v, load_sem.at[3])
    load_dy.start()
    load_wd.start()
    pl.semaphore_wait(barrier, 3)

    gy.start(R0, L1, OWN, R1, L0)
    load_x.start()
    load_wi.start()
    give_w = pltpu.make_async_remote_copy(
        src_ref=w_in, dst_ref=wp_v, send_sem=w_send, recv_sem=w_recv,
        device_id=to_partner, device_id_type=pl.DeviceIdType.MESH,
    )
    give_w.start()

    load_dy.wait()
    keep_dy = pltpu.make_async_copy(dy_v.at[first], block(dyg, chip, core), store_sem.at[0])
    keep_dy.start()
    load_x.wait()
    keep_x = pltpu.make_async_copy(low_v, block(xg, chip, core), store_sem.at[1])
    keep_x.start()
    load_wd.wait()
    load_wi.wait()

    def chip_of(stage):
        return lax.rem(chip + jnp.where(stage == 0, 0, jnp.where(stage == 1, chips - 1, stage - 1)), chips)

    def hidden_grad(stage, k, out_v):
        c = chip_of(stage)
        load_pre = pltpu.make_async_copy(block(pre, c, k), pre_v.at[first], load_sem.at[0])
        load_pre.start()
        load = pltpu.make_async_copy(block(dyg, c, k), dy_v.at[first], load_sem.at[1])
        load.start()
        load.wait()
        load_pre.wait()

        @pl.loop(0, cols // tile)
        def _(t):
            span = pl.ds(pl.multiple_of(t * tile, tile), tile)
            grad = lax.dot_general(dy_v[first, :], wd_v[span, :], NT, preferred_element_type=F32)
            p = pre_v[first, span].astype(F32)
            out_v[:, span] = jnp.where(p > 0, grad * (2.0 * p), 0.0).astype(BF16)

        keep = pltpu.make_async_copy(out_v, block(d_pre, c, k), store_sem.at[2])
        keep.start()
        return keep

    def swap(stage):
        return pltpu.make_async_remote_copy(
            src_ref=other_v, dst_ref=got_v.at[stage], send_sem=got_send, recv_sem=got_recv.at[stage],
            device_id=to_partner, device_id_type=pl.DeviceIdType.MESH,
        )

    keep_dy.wait()
    keep_x.wait()
    dw_v[...] = jnp.zeros_like(dw_v)

    cut = half // 32 * 16 + 16
    pieces = [(0, cut, to_right), (cut, half - cut, to_right), (half, cut, to_left), (half + cut, half - cut, to_left)]

    def far_piece(i):
        start, size, target = pieces[i]
        span = pl.ds(start, size)
        return pltpu.make_async_remote_copy(
            src_ref=low_v.at[span], dst_ref=far_v.at[span], send_sem=far_send.at[i], recv_sem=far_recv.at[i],
            device_id=target, device_id_type=pl.DeviceIdType.MESH,
        )

    def put(src, dst, i):
        copy = pltpu.make_async_copy(src, dst, store_sem.at[i])
        copy.start()
        return copy

    @pl.loop(0, chips)
    def _(stage):
        @pl.when(stage == 1)
        def _():
            gy.arrived(R0, L1)
            gy.start(FR, FL, PL0, PR1)
            gx.start(R0, L1, R1, L0, OWN)
            gy.arrived(R1, L0)
            gy.start(PL1, PR0)

        @pl.when(stage == 3)
        def _():
            gy.arrived(FR, FL)
            gy.start(PO0, PO1)

        hidden_grad(stage, core, mine_v).wait()

        @pl.when(stage == 0)
        def _():
            gy.arrived(OWN)

        @pl.when(stage == 1)
        def _():
            gy.arrived(PL0, PL1)

        @pl.when(stage == 2)
        def _():
            gy.arrived(PR0, PR1)

        @pl.when(stage == 3)
        def _():
            gy.arrived(PO0, PO1)

        keep = hidden_grad(stage, 1 - core, other_v)
        give = swap(stage)
        give.start()

        @pl.when(stage == 0)
        def _():
            give_w.wait()

        @pl.when(stage == 3)
        def _():
            gx.arrived(R0, L1)
            gx.start(FR, FL, PL0, PR1)

        give.wait_recv()
        wide = 512

        @pl.loop(0, depth // wide)
        def _(t):
            span = pl.ds(pl.multiple_of(t * wide, wide), wide)
            term = lax.dot_general(mine_v[...], wi_v[span, :], NT, preferred_element_type=F32)
            term += lax.dot_general(got_v[stage], wp_v[span, :], NT, preferred_element_type=F32)
            acc_v[:, span] = term
            low_v[:, span] = term.astype(BF16)

        give.wait_send()
        keep.wait()

        @pl.when(stage == 0)
        def _():
            put(acc_v, s_own, 3).wait()

        @pl.when(stage == 1)
        def _():
            wait_v[bottom, :] = acc_v[bottom, :]
            put(low_v.at[top], go_left.at[top], 3).wait()

        @pl.when(stage == 2)
        def _():
            wait_v[top, :] = acc_v[top, :]
            put(low_v.at[bottom], go_right.at[bottom], 3).wait()

    for i in (0, 2, 1, 3):
        far_piece(i).start()

    @pl.loop(0, chips)
    def _(stage):
        span = pl.ds(pl.multiple_of(chip_of(stage) * CORES * rows, 16), CORES * rows)
        load_pre = pltpu.make_async_copy(pre.at[span], pre_v, load_sem.at[0])
        load = pltpu.make_async_copy(dyg.at[span], dy_v, load_sem.at[1])
        load_pre.start()
        load.start()
        load_pre.wait()

        @pl.loop(0, cols // tile)
        def _(m):
            ms = pl.ds(pl.multiple_of(m * tile, tile), tile)
            pair_v[:, ms] = jnp.square(jnp.maximum(pre_v[:, ms].astype(F32), 0.0)).astype(BF16)

        load.wait()

        @pl.loop(0, cols // tile)
        def _(m):
            ms = pl.ds(pl.multiple_of(m * tile, tile), tile)

            @pl.loop(0, CORES)
            def _(t):
                wide = depth // CORES
                ns = pl.ds(pl.multiple_of(t * wide, wide), wide)
                dw_v[ms, ns] += lax.dot_general(pair_v[:, ms], dy_v[:, ns], TN, preferred_element_type=F32)

    @pl.loop(0, cols // tile)
    def _(m):
        ms = pl.ds(pl.multiple_of(m * tile, tile), tile)
        wd_v[ms, :] = dw_v[ms, :].astype(BF16)

    put_dw = put(wd_v, dw_down, 4)

    gx.arrived(R1, L0)
    gx.start(PL1, PR0)
    gx.arrived(FR, FL)
    gx.start(PO0, PO1)
    gx.arrived(OWN, PL0, PL1, PR0, PR1, PO0, PO1)
    gy.sent()
    gx.sent()

    puts = []
    for i in (0, 2, 1, 3):
        start, size, _ = pieces[i]
        span = pl.ds(start, size)
        far_piece(i).wait()
        dy_v[span, :] = (wait_v[span, :] + far_v[span, :].astype(F32)).astype(BF16)
        puts.append(put(dy_v.at[span], (go_right if i < 2 else go_left).at[span], i))
    for copy in puts:
        copy.wait()
    put_dw.wait()


def solution(mesh):
    n = mesh.shape["tp"]
    chips = n // CORES

    def gather(x, dy, pre, w_in, w_down):
        rows, depth = x.shape
        tokens, cols = pre.shape
        anywhere = pl.BlockSpec(memory_space=pl.ANY)
        shape = jax.ShapeDtypeStruct
        return pl.pallas_call(
            functools.partial(gather_kernel, chips),
            name="gather",
            out_shape=(
                shape((tokens, depth), BF16),
                shape((tokens, depth), BF16),
                shape((tokens, cols), BF16),
                shape((rows, depth), F32),
                shape((rows, depth), BF16),
                shape((rows, depth), BF16),
                shape((cols, depth), BF16),
            ),
            in_specs=[anywhere] * 5,
            out_specs=(anywhere,) * 7,
            scratch_shapes=[
                pltpu.VMEM((cols, depth), BF16),
                pltpu.VMEM((depth, cols), BF16),
                pltpu.VMEM((depth, cols), BF16),
                pltpu.VMEM((CORES * rows, depth), BF16),
                pltpu.VMEM((CORES * rows, cols), BF16),
                pltpu.VMEM((CORES * rows, cols), BF16),
                pltpu.VMEM((chips, rows, cols), BF16),
                pltpu.VMEM((rows, depth), F32),
                pltpu.VMEM((rows, depth), BF16),
                pltpu.VMEM((rows, depth), F32),
                pltpu.VMEM((rows, depth), BF16),
                pltpu.VMEM((cols, depth), F32),
                pltpu.SemaphoreType.DMA((2, COPIES)),
                pltpu.SemaphoreType.DMA((2, COPIES)),
                pltpu.SemaphoreType.DMA,
                pltpu.SemaphoreType.DMA((chips,)),
                pltpu.SemaphoreType.DMA,
                pltpu.SemaphoreType.DMA,
                pltpu.SemaphoreType.DMA((4,)),
                pltpu.SemaphoreType.DMA((4,)),
                pltpu.SemaphoreType.DMA((4,)),
                pltpu.SemaphoreType.DMA((5,)),
            ],
            compiler_params=pltpu.CompilerParams(
                collective_id=0, has_side_effects=True, vmem_limit_bytes=64 * 1024 * 1024 - 65536
            ),
            cost_estimate=pl.CostEstimate(
                flops=6 * tokens * depth * cols, bytes_accessed=8 * tokens * depth, transcendentals=0
            ),
        )(x, dy, pre, w_in, w_down)

    def hand_on(a):
        rows, depth = a.shape
        spec = pl.BlockSpec((rows // 8, depth), lambda i: (i, 0))

        def body(a_ref, out_ref):
            out_ref[...] = a_ref[...]

        return pl.pallas_call(
            body, name="hand_on", grid=(8,), in_specs=[spec], out_specs=spec, out_shape=jax.ShapeDtypeStruct(a.shape, a.dtype),
            cost_estimate=pl.CostEstimate(flops=rows * depth * 64, bytes_accessed=4 * rows * depth, transcendentals=0),
        )(a)

    def step(x, dy, pre, w_in, w_down):
        clockwise = [(i, (i + CORES) % n) for i in range(n)]
        counter = [(i, (i - CORES) % n) for i in range(n)]
        xg, dyg, d_pre, s_own, go_left, go_right, dw_down = gather(x, dy, pre, w_in, w_down)
        from_left = lax.ppermute(go_right, "tp", clockwise)
        from_right = lax.ppermute(go_left, "tp", counter)
        dw_in = lax.dot_general(xg, d_pre, TN, preferred_element_type=F32).astype(BF16)
        dw_down = hand_on(dw_down)
        s_own, dw_in, dw_down = lax.optimization_barrier((s_own, dw_in, dw_down))
        dx = (s_own + from_left.astype(F32) + from_right.astype(F32)).astype(BF16)
        return dx, dw_in, dw_down

    tokens, columns, weight_rows = P(("dp", "tp"), None), P(None, "tp"), P("tp", None)
    return jax.shard_map(
        step,
        mesh=mesh,
        in_specs=(tokens, tokens, P("dp", "tp"), columns, weight_rows),
        out_specs=(tokens, P("dp", "tp"), P(("dp", "tp"), None)),
        check_vma=False,
    )
```

```python
import functools

import jax
import jax.numpy as jnp
from jax import lax
from jax.experimental import pallas as pl
from jax.experimental.pallas import tpu as pltpu
from jax.sharding import PartitionSpec as P

CORES = 2
LATE = 64
F32, BF16 = jnp.float32, jnp.bfloat16
NT = (((1,), (1,)), ((), ()))
TN = (((0,), (0,)), ((), ()))

(R0, R1, L0, L1, OWN, FR, FL, PL0, PL1, PR0, PR1, PO0, PO1) = range(13)
COPIES = 13


def gather_kernel(
    chips, x, dy, pre, w_in, w_down,
    xg, dyg, d_pre, s_own, go_left, go_left_late, go_right, go_right_late, dw_down,
    wd_v, wi_v, wp_v, dy_v, pre_v, pair_v, got_v, acc_v, low_v, wait_v, far_v, dw_v,
    send_sem, recv_sem, got_send, got_recv, w_send, w_recv, far_send, far_recv, load_sem, store_sem,
):
    rows, depth = dy.shape
    half = rows // 2
    cols = w_down.shape[0]
    tile = 384
    first, top, bottom = pl.ds(0, rows), pl.ds(0, half), pl.ds(half, half)
    mine_v, other_v = pair_v.at[first], pair_v.at[pl.ds(rows, rows)]
    me = lax.axis_index("tp")
    chip, core = me // CORES, lax.rem(me, CORES)
    left = lax.rem(chip + chips - 1, chips)
    right = lax.rem(chip + 1, chips)
    far = lax.rem(chip + 2, chips)

    def device(c, k):
        return {"tp": c * CORES + k}

    to_right, to_left, to_partner = device(right, core), device(left, core), device(chip, 1 - core)

    def block(ref, c, k, h=None):
        start = (c * CORES + k) * rows
        if h is None:
            return ref.at[pl.ds(pl.multiple_of(start, 16), rows)]
        return ref.at[pl.ds(pl.multiple_of(start + h * half, 16), half)]

    class Gather:
        def __init__(self, which, src, dst):
            self.which, self.src, self.dst = which, src, dst

        def own(self, h):
            return self.src.at[pl.ds(h * half, half)]

        def copy(self, n, src, dst, target):
            return pltpu.make_async_remote_copy(
                src_ref=src, dst_ref=dst, send_sem=send_sem.at[self.which, n], recv_sem=recv_sem.at[self.which, n],
                device_id=target, device_id_type=pl.DeviceIdType.MESH,
            )

        def out(self, n):
            d = self.dst
            if n in (R0, R1):
                h = n - R0
                return self.copy(n, self.own(h), block(d, chip, core, h), to_right)
            if n in (L0, L1):
                h = n - L0
                return self.copy(n, self.own(h), block(d, chip, core, h), to_left)
            if n == OWN:
                return self.copy(n, self.src, block(d, chip, core), to_partner)
            if n == FR:
                return self.copy(n, block(d, left, core, 0), block(d, left, core, 0), to_right)
            if n == FL:
                return self.copy(n, block(d, right, core, 1), block(d, right, core, 1), to_left)
            c, h = {PL0: (left, 0), PL1: (left, 1), PR0: (right, 0), PR1: (right, 1), PO0: (far, 0), PO1: (far, 1)}[n]
            return self.copy(n, block(d, c, core, h), block(d, c, core, h), to_partner)

        def start(self, *names):
            for n in names:
                self.out(n).start()

        def arrived(self, *names):
            for n in names:
                if n == OWN:
                    dst = block(self.dst, chip, 1 - core)
                else:
                    c, k, h = {
                        R0: (left, core, 0), R1: (left, core, 1), L0: (right, core, 0), L1: (right, core, 1),
                        FR: (far, core, 0), FL: (far, core, 1),
                        PL0: (left, 1 - core, 0), PL1: (left, 1 - core, 1), PR0: (right, 1 - core, 0),
                        PR1: (right, 1 - core, 1), PO0: (far, 1 - core, 0), PO1: (far, 1 - core, 1),
                    }[n]
                    dst = block(self.dst, c, k, h)
                self.copy(n, dst, dst, to_partner).wait_recv()

        def sent(self):
            for n in range(COPIES):
                self.out(n).wait_send()

    gy, gx = Gather(0, dy, dyg), Gather(1, x, xg)

    barrier = pltpu.get_barrier_semaphore()
    for target in (to_right, to_left, to_partner):
        pl.semaphore_signal(barrier, inc=1, device_id=target, device_id_type=pl.DeviceIdType.MESH)
    load_wd = pltpu.make_async_copy(w_down, wd_v, load_sem.at[0])
    load_dy = pltpu.make_async_copy(dy, dy_v.at[first], load_sem.at[1])
    load_x = pltpu.make_async_copy(x, low_v, load_sem.at[2])
    load_wi = pltpu.make_async_copy(w_in, wi_v, load_sem.at[3])
    load_dy.start()
    load_wd.start()
    pl.semaphore_wait(barrier, 3)

    gy.start(R0, L1, OWN, R1, L0)
    gx.start(R0, L1)
    load_x.start()
    load_wi.start()
    give_w = pltpu.make_async_remote_copy(
        src_ref=w_in, dst_ref=wp_v, send_sem=w_send, recv_sem=w_recv,
        device_id=to_partner, device_id_type=pl.DeviceIdType.MESH,
    )
    give_w.start()

    load_dy.wait()
    keep_dy = pltpu.make_async_copy(dy_v.at[first], block(dyg, chip, core), store_sem.at[0])
    keep_dy.start()
    load_x.wait()
    keep_x = pltpu.make_async_copy(low_v, block(xg, chip, core), store_sem.at[1])
    keep_x.start()
    load_wd.wait()
    load_wi.wait()

    def chip_of(stage):
        return lax.rem(chip + jnp.where(stage == 0, 0, jnp.where(stage == 1, chips - 1, stage - 1)), chips)

    def hidden_grad(stage, k, out_v):
        c = chip_of(stage)
        load_pre = pltpu.make_async_copy(block(pre, c, k), pre_v.at[first], load_sem.at[0])
        load_pre.start()
        load = pltpu.make_async_copy(block(dyg, c, k), dy_v.at[first], load_sem.at[1])
        load.start()
        load.wait()
        load_pre.wait()

        @pl.loop(0, cols // tile)
        def _(t):
            span = pl.ds(pl.multiple_of(t * tile, tile), tile)
            grad = lax.dot_general(dy_v[first, :], wd_v[span, :], NT, preferred_element_type=F32)
            p = pre_v[first, span].astype(F32)
            out_v[:, span] = jnp.where(p > 0, grad * (2.0 * p), 0.0).astype(BF16)

        keep = pltpu.make_async_copy(out_v, block(d_pre, c, k), store_sem.at[2])
        keep.start()
        return keep

    def swap(stage):
        return pltpu.make_async_remote_copy(
            src_ref=other_v, dst_ref=got_v.at[stage], send_sem=got_send, recv_sem=got_recv.at[stage],
            device_id=to_partner, device_id_type=pl.DeviceIdType.MESH,
        )

    keep_dy.wait()
    keep_x.wait()
    dw_v[...] = jnp.zeros_like(dw_v)

    cut = half - (rows - go_left.shape[0])
    pieces = [(0, cut, to_right), (cut, half - cut, to_right), (half, cut, to_left), (half + cut, half - cut, to_left)]

    def far_piece(i):
        start, size, target = pieces[i]
        span = pl.ds(start, size)
        return pltpu.make_async_remote_copy(
            src_ref=low_v.at[span], dst_ref=far_v.at[span], send_sem=far_send.at[i], recv_sem=far_recv.at[i],
            device_id=target, device_id_type=pl.DeviceIdType.MESH,
        )

    def put(src, dst, i):
        copy = pltpu.make_async_copy(src, dst, store_sem.at[i])
        copy.start()
        return copy

    @pl.loop(0, chips)
    def _(stage):
        @pl.when(stage == 1)
        def _():
            gy.arrived(R0, L1)
            gy.start(FR, FL, PL0, PR1)
            gx.start(R1, L0, OWN)
            gy.arrived(R1, L0)
            gy.start(PL1, PR0)

        @pl.when(stage == 3)
        def _():
            gx.arrived(R0, L1)
            gx.start(FR, FL, PL0, PR1)
            gy.arrived(FR, FL)
            gy.start(PO0, PO1)

        hidden_grad(stage, core, mine_v).wait()

        @pl.when(stage == 0)
        def _():
            gy.arrived(OWN)

        @pl.when(stage == 1)
        def _():
            gy.arrived(PL0, PL1)

        @pl.when(stage == 2)
        def _():
            gy.arrived(PR0, PR1)

        @pl.when(stage == 3)
        def _():
            gy.arrived(PO0, PO1)

        keep = hidden_grad(stage, 1 - core, other_v)
        give = swap(stage)
        give.start()

        @pl.when(stage == 0)
        def _():
            give_w.wait()

        give.wait_recv()
        wide = 512

        @pl.loop(0, depth // wide)
        def _(t):
            span = pl.ds(pl.multiple_of(t * wide, wide), wide)
            term = lax.dot_general(mine_v[...], wi_v[span, :], NT, preferred_element_type=F32)
            term += lax.dot_general(got_v[stage], wp_v[span, :], NT, preferred_element_type=F32)
            acc_v[:, span] = term
            low_v[:, span] = term.astype(BF16)

        give.wait_send()
        keep.wait()

        @pl.when(stage == 0)
        def _():
            put(acc_v, s_own, 3).wait()

        @pl.when(stage == 1)
        def _():
            wait_v[bottom, :] = acc_v[bottom, :]
            put(low_v.at[top], go_left.at[top], 3).wait()

        @pl.when(stage == 2)
        def _():
            wait_v[top, :] = acc_v[top, :]
            early = go_right.shape[0]
            a = put(low_v.at[pl.ds(half, early - half)], go_right.at[pl.ds(half, early - half)], 3)
            b = put(low_v.at[pl.ds(early, rows - early)], go_right_late, 2)
            a.wait()
            b.wait()

    for i in (0, 2, 1, 3):
        far_piece(i).start()

    @pl.loop(0, chips)
    def _(stage):
        span = pl.ds(pl.multiple_of(chip_of(stage) * CORES * rows, 16), CORES * rows)
        load_pre = pltpu.make_async_copy(pre.at[span], pre_v, load_sem.at[0])
        load = pltpu.make_async_copy(dyg.at[span], dy_v, load_sem.at[1])
        load_pre.start()
        load.start()
        load_pre.wait()

        @pl.loop(0, cols // tile)
        def _(m):
            ms = pl.ds(pl.multiple_of(m * tile, tile), tile)
            pair_v[:, ms] = jnp.square(jnp.maximum(pre_v[:, ms].astype(F32), 0.0)).astype(BF16)

        load.wait()

        @pl.loop(0, cols // tile)
        def _(m):
            ms = pl.ds(pl.multiple_of(m * tile, tile), tile)

            @pl.loop(0, CORES)
            def _(t):
                wide = depth // CORES
                ns = pl.ds(pl.multiple_of(t * wide, wide), wide)
                dw_v[ms, ns] += lax.dot_general(pair_v[:, ms], dy_v[:, ns], TN, preferred_element_type=F32)

    @pl.loop(0, cols // tile)
    def _(m):
        ms = pl.ds(pl.multiple_of(m * tile, tile), tile)
        wd_v[ms, :] = dw_v[ms, :].astype(BF16)

    put_dw = put(wd_v, dw_down, 4)

    gx.arrived(R1, L0)
    gx.start(PL1, PR0)
    gx.arrived(FR, FL)
    gx.start(PO0, PO1)
    gx.arrived(OWN, PL0, PL1, PR0, PR1, PO0, PO1)
    gy.sent()
    gx.sent()

    puts = []
    for i in (0, 2, 1, 3):
        start, size, _ = pieces[i]
        span = pl.ds(start, size)
        far_piece(i).wait()
        dy_v[span, :] = (wait_v[span, :] + far_v[span, :].astype(F32)).astype(BF16)
        target = go_left_late if i == 3 else (go_right if i < 2 else go_left).at[span]
        puts.append(put(dy_v.at[span], target, i))
    for copy in puts:
        copy.wait()
    put_dw.wait()


def solution(mesh):
    n = mesh.shape["tp"]
    chips = n // CORES

    def gather(x, dy, pre, w_in, w_down):
        rows, depth = x.shape
        tokens, cols = pre.shape
        early = rows - LATE
        anywhere = pl.BlockSpec(memory_space=pl.ANY)
        shape = jax.ShapeDtypeStruct
        return pl.pallas_call(
            functools.partial(gather_kernel, chips),
            name="gather",
            out_shape=(
                shape((tokens, depth), BF16),
                shape((tokens, depth), BF16),
                shape((tokens, cols), BF16),
                shape((rows, depth), F32),
                shape((early, depth), BF16),
                shape((rows - early, depth), BF16),
                shape((early, depth), BF16),
                shape((rows - early, depth), BF16),
                shape((cols, depth), BF16),
            ),
            in_specs=[anywhere] * 5,
            out_specs=(anywhere,) * 9,
            scratch_shapes=[
                pltpu.VMEM((cols, depth), BF16),
                pltpu.VMEM((depth, cols), BF16),
                pltpu.VMEM((depth, cols), BF16),
                pltpu.VMEM((CORES * rows, depth), BF16),
                pltpu.VMEM((CORES * rows, cols), BF16),
                pltpu.VMEM((CORES * rows, cols), BF16),
                pltpu.VMEM((chips, rows, cols), BF16),
                pltpu.VMEM((rows, depth), F32),
                pltpu.VMEM((rows, depth), BF16),
                pltpu.VMEM((rows, depth), F32),
                pltpu.VMEM((rows, depth), BF16),
                pltpu.VMEM((cols, depth), F32),
                pltpu.SemaphoreType.DMA((2, COPIES)),
                pltpu.SemaphoreType.DMA((2, COPIES)),
                pltpu.SemaphoreType.DMA,
                pltpu.SemaphoreType.DMA((chips,)),
                pltpu.SemaphoreType.DMA,
                pltpu.SemaphoreType.DMA,
                pltpu.SemaphoreType.DMA((4,)),
                pltpu.SemaphoreType.DMA((4,)),
                pltpu.SemaphoreType.DMA((4,)),
                pltpu.SemaphoreType.DMA((5,)),
            ],
            compiler_params=pltpu.CompilerParams(
                collective_id=0, has_side_effects=True, vmem_limit_bytes=64 * 1024 * 1024 - 65536
            ),
            cost_estimate=pl.CostEstimate(
                flops=6 * tokens * depth * cols, bytes_accessed=8 * tokens * depth, transcendentals=0
            ),
        )(x, dy, pre, w_in, w_down)

    def hand_on(a):
        rows, depth = a.shape
        spec = pl.BlockSpec((rows // 8, depth), lambda i: (i, 0))

        def body(a_ref, out_ref):
            out_ref[...] = a_ref[...]

        return pl.pallas_call(
            body, name="hand_on", grid=(8,), in_specs=[spec], out_specs=spec, out_shape=jax.ShapeDtypeStruct(a.shape, a.dtype),
            cost_estimate=pl.CostEstimate(flops=rows * depth * 64, bytes_accessed=4 * rows * depth, transcendentals=0),
        )(a)

    def add_kernel(own, one, other, *refs):
        refs[-1][...] = (own[...] + one[...].astype(F32) + other[...].astype(F32)).astype(BF16)

    def final_sum(own, one, other, start, block, so_far=None):
        rows, depth = own.shape
        moved = pl.BlockSpec((block, depth), lambda i: (start // block + i, 0))
        plain = pl.BlockSpec((block, depth), lambda i: (i, 0))
        before = [] if so_far is None else [so_far]
        return pl.pallas_call(
            add_kernel, name="final_sum", grid=(one.shape[0] // block,),
            in_specs=[moved, plain, plain] + [pl.BlockSpec(memory_space=pl.ANY) for _ in before],
            out_specs=moved, out_shape=jax.ShapeDtypeStruct((rows, depth), BF16),
            input_output_aliases={3: 0} if before else {},
            cost_estimate=pl.CostEstimate(flops=one.size * 64, bytes_accessed=10 * one.size, transcendentals=0),
        )(own, one, other, *before)

    def step(x, dy, pre, w_in, w_down):
        clockwise = [(i, (i + CORES) % n) for i in range(n)]
        counter = [(i, (i - CORES) % n) for i in range(n)]
        xg, dyg, d_pre, s_own, go_left, go_left_late, go_right, go_right_late, dw_down = gather(x, dy, pre, w_in, w_down)
        from_left = lax.ppermute(go_right, "tp", clockwise)
        from_right = lax.ppermute(go_left, "tp", counter)
        from_left_late = lax.ppermute(go_right_late, "tp", clockwise)
        from_right_late = lax.ppermute(go_left_late, "tp", counter)
        dw_in = lax.dot_general(xg, d_pre, TN, preferred_element_type=F32).astype(BF16)
        dw_down = hand_on(dw_down)
        s_own, dw_in, dw_down = lax.optimization_barrier((s_own, dw_in, dw_down))
        dx = final_sum(s_own, from_left, from_right, 0, 96)
        dx = final_sum(s_own, from_left_late, from_right_late, from_left.shape[0], 32, dx)
        return dx, dw_in, dw_down

    tokens, columns, weight_rows = P(("dp", "tp"), None), P(None, "tp"), P("tp", None)
    return jax.shard_map(
        step,
        mesh=mesh,
        in_specs=(tokens, tokens, P("dp", "tp"), columns, weight_rows),
        out_specs=(tokens, P("dp", "tp"), P(("dp", "tp"), None)),
        check_vma=False,
    )
```

```python
import functools

import jax
import jax.numpy as jnp
from jax import lax
from jax.experimental import pallas as pl
from jax.experimental.pallas import tpu as pltpu
from jax.sharding import PartitionSpec as P


CORES = 2
LATE, EDGE = 64, 32
F32, BF16 = jnp.float32, jnp.bfloat16
NT = (((1,), (1,)), ((), ()))
TN = (((0,), (0,)), ((), ()))

(R0, R1, L0, L1, OWN, FR, FL, PL0, PL1, PR0, PR1, PO0, PO1) = range(13)
COPIES = 13


def gather_kernel(
    chips, x, dy, pre, w_in, w_down,
    xg, dyg, d_pre, s_own, s_own_late, go_left, go_left_late, go_right, go_right_late, got_left, got_right, dw_down,
    wd_v, wi_v, wp_v, dy_v, pre_v, pair_v, got_v, acc_v, low_v, wait_v, far_v, hold_v, dw_v,
    send_sem, recv_sem, got_send, got_recv, w_send, w_recv, far_send, far_recv, hold_send, hold_recv, load_sem, store_sem,
):
    rows, depth = dy.shape
    half = rows // 2
    cols = w_down.shape[0]
    tile = 384
    first, top, bottom = pl.ds(0, rows), pl.ds(0, half), pl.ds(half, half)
    mine_v, other_v = pair_v.at[first], pair_v.at[pl.ds(rows, rows)]
    me = lax.axis_index("tp")
    chip, core = me // CORES, lax.rem(me, CORES)
    left = lax.rem(chip + chips - 1, chips)
    right = lax.rem(chip + 1, chips)
    far = lax.rem(chip + 2, chips)

    def device(c, k):
        return {"tp": c * CORES + k}

    to_right, to_left, to_partner = device(right, core), device(left, core), device(chip, 1 - core)

    def block(ref, c, k, h=None):
        start = (c * CORES + k) * rows
        if h is None:
            return ref.at[pl.ds(pl.multiple_of(start, 16), rows)]
        return ref.at[pl.ds(pl.multiple_of(start + h * half, 16), half)]

    class Gather:
        def __init__(self, which, src, dst):
            self.which, self.src, self.dst = which, src, dst

        def own(self, h):
            return self.src.at[pl.ds(h * half, half)]

        def copy(self, n, src, dst, target):
            return pltpu.make_async_remote_copy(
                src_ref=src, dst_ref=dst, send_sem=send_sem.at[self.which, n], recv_sem=recv_sem.at[self.which, n],
                device_id=target, device_id_type=pl.DeviceIdType.MESH,
            )

        def out(self, n):
            d = self.dst
            if n in (R0, R1):
                h = n - R0
                return self.copy(n, self.own(h), block(d, chip, core, h), to_right)
            if n in (L0, L1):
                h = n - L0
                return self.copy(n, self.own(h), block(d, chip, core, h), to_left)
            if n == OWN:
                return self.copy(n, self.src, block(d, chip, core), to_partner)
            if n == FR:
                return self.copy(n, block(d, left, core, 0), block(d, left, core, 0), to_right)
            if n == FL:
                return self.copy(n, block(d, right, core, 1), block(d, right, core, 1), to_left)
            c, h = {PL0: (left, 0), PL1: (left, 1), PR0: (right, 0), PR1: (right, 1), PO0: (far, 0), PO1: (far, 1)}[n]
            return self.copy(n, block(d, c, core, h), block(d, c, core, h), to_partner)

        def start(self, *names):
            for n in names:
                self.out(n).start()

        def arrived(self, *names):
            for n in names:
                if n == OWN:
                    dst = block(self.dst, chip, 1 - core)
                else:
                    c, k, h = {
                        R0: (left, core, 0), R1: (left, core, 1), L0: (right, core, 0), L1: (right, core, 1),
                        FR: (far, core, 0), FL: (far, core, 1),
                        PL0: (left, 1 - core, 0), PL1: (left, 1 - core, 1), PR0: (right, 1 - core, 0),
                        PR1: (right, 1 - core, 1), PO0: (far, 1 - core, 0), PO1: (far, 1 - core, 1),
                    }[n]
                    dst = block(self.dst, c, k, h)
                self.copy(n, dst, dst, to_partner).wait_recv()

        def sent(self):
            for n in range(COPIES):
                self.out(n).wait_send()

    gy, gx = Gather(0, dy, dyg), Gather(1, x, xg)

    barrier = pltpu.get_barrier_semaphore()
    for target in (to_right, to_left, to_partner):
        pl.semaphore_signal(barrier, inc=1, device_id=target, device_id_type=pl.DeviceIdType.MESH)
    load_wd = pltpu.make_async_copy(w_down, wd_v, load_sem.at[0])
    load_dy = pltpu.make_async_copy(dy, dy_v.at[first], load_sem.at[1])
    load_x = pltpu.make_async_copy(x, low_v, load_sem.at[2])
    load_wi = pltpu.make_async_copy(w_in, wi_v, load_sem.at[3])
    load_dy.start()
    load_wd.start()
    pl.semaphore_wait(barrier, 3)

    gy.start(R0, L1, OWN, R1, L0)
    gx.start(R0, L1)
    load_x.start()
    load_wi.start()
    give_w = pltpu.make_async_remote_copy(
        src_ref=w_in, dst_ref=wp_v, send_sem=w_send, recv_sem=w_recv,
        device_id=to_partner, device_id_type=pl.DeviceIdType.MESH,
    )
    give_w.start()

    load_dy.wait()
    keep_dy = pltpu.make_async_copy(dy_v.at[first], block(dyg, chip, core), store_sem.at[0])
    keep_dy.start()
    load_x.wait()
    keep_x = pltpu.make_async_copy(low_v, block(xg, chip, core), store_sem.at[1])
    keep_x.start()
    load_wd.wait()
    load_wi.wait()

    def chip_of(stage):
        return lax.rem(chip + jnp.where(stage == 0, 0, jnp.where(stage == 1, chips - 1, stage - 1)), chips)

    def hidden_grad(stage, k, out_v):
        c = chip_of(stage)
        load_pre = pltpu.make_async_copy(block(pre, c, k), pre_v.at[first], load_sem.at[0])
        load_pre.start()
        load = pltpu.make_async_copy(block(dyg, c, k), dy_v.at[first], load_sem.at[1])
        load.start()
        load.wait()
        load_pre.wait()

        @pl.loop(0, cols // tile)
        def _(t):
            span = pl.ds(pl.multiple_of(t * tile, tile), tile)
            grad = lax.dot_general(dy_v[first, :], wd_v[span, :], NT, preferred_element_type=F32)
            p = pre_v[first, span].astype(F32)
            out_v[:, span] = jnp.where(p > 0, grad * (2.0 * p), 0.0).astype(BF16)

        keep = pltpu.make_async_copy(out_v, block(d_pre, c, k), store_sem.at[2])
        keep.start()
        return keep

    def swap(stage):
        return pltpu.make_async_remote_copy(
            src_ref=other_v, dst_ref=got_v.at[stage], send_sem=got_send, recv_sem=got_recv.at[stage],
            device_id=to_partner, device_id_type=pl.DeviceIdType.MESH,
        )

    keep_dy.wait()
    keep_x.wait()
    dw_v[...] = jnp.zeros_like(dw_v)

    edge, late = got_left.shape[0], go_left_late.shape[0]
    mid, end = rows - edge - late, rows - edge
    cut = half // 32 * 16
    pieces = [
        (0, cut, to_right, go_right.at[pl.ds(0, cut)]),
        (cut, half - cut, to_right, go_right.at[pl.ds(cut, half - cut)]),
        (half, mid - half, to_left, go_left.at[pl.ds(half - edge, mid - half)]),
        (mid, late, to_left, go_left_late),
        (end, edge, to_left, go_left.at[pl.ds(mid - edge, edge)]),
    ]
    order = (0, 2, 1, 3, 4)

    def far_piece(i):
        start, size, target, _ = pieces[i]
        span = pl.ds(start, size)
        return pltpu.make_async_remote_copy(
            src_ref=low_v.at[span], dst_ref=far_v.at[span], send_sem=far_send.at[i], recv_sem=far_recv.at[i],
            device_id=target, device_id_type=pl.DeviceIdType.MESH,
        )

    def held_piece(i):
        return pltpu.make_async_remote_copy(
            src_ref=hold_v.at[pl.ds(i * edge, edge)], dst_ref=(got_right, got_left)[i],
            send_sem=hold_send.at[i], recv_sem=hold_recv.at[i],
            device_id=(to_left, to_right)[i], device_id_type=pl.DeviceIdType.MESH,
        )

    def put(src, dst, i):
        copy = pltpu.make_async_copy(src, dst, store_sem.at[i])
        copy.start()
        return copy

    @pl.loop(0, chips)
    def _(stage):
        @pl.when(stage == 1)
        def _():
            gy.arrived(R0, L1)
            gy.start(FR, FL, PL0, PR1)
            gx.start(R1, L0, OWN)
            gy.arrived(R1, L0)
            gy.start(PL1, PR0)

        @pl.when(stage == 3)
        def _():
            gx.arrived(R0, L1)
            gx.start(FR, FL, PL0, PR1)
            gy.arrived(FR, FL)
            gy.start(PO0, PO1)

        hidden_grad(stage, core, mine_v).wait()

        @pl.when(stage == 0)
        def _():
            gy.arrived(OWN)

        @pl.when(stage == 1)
        def _():
            gy.arrived(PL0, PL1)

        @pl.when(stage == 2)
        def _():
            gy.arrived(PR0, PR1)

        @pl.when(stage == 3)
        def _():
            gy.arrived(PO0, PO1)

        keep = hidden_grad(stage, 1 - core, other_v)
        give = swap(stage)
        give.start()

        @pl.when(stage == 0)
        def _():
            give_w.wait()

        give.wait_recv()
        wide = 512

        @pl.loop(0, depth // wide)
        def _(t):
            span = pl.ds(pl.multiple_of(t * wide, wide), wide)
            term = lax.dot_general(mine_v[...], wi_v[span, :], NT, preferred_element_type=F32)
            term += lax.dot_general(got_v[stage], wp_v[span, :], NT, preferred_element_type=F32)
            acc_v[:, span] = term
            low_v[:, span] = term.astype(BF16)

        give.wait_send()
        keep.wait()

        @pl.when(stage == 0)
        def _():
            puts = [
                put(acc_v.at[pl.ds(0, mid)], s_own.at[pl.ds(0, mid)], 1),
                put(acc_v.at[pl.ds(mid, late)], s_own_late, 2),
                put(acc_v.at[pl.ds(end, edge)], s_own.at[pl.ds(mid, edge)], 3),
            ]
            for copy in puts:
                copy.wait()

        @pl.when(stage == 1)
        def _():
            wait_v[bottom, :] = acc_v[bottom, :]
            hold_v[pl.ds(0, edge), :] = low_v[pl.ds(0, edge), :]
            put(low_v.at[pl.ds(edge, half - edge)], go_left.at[pl.ds(0, half - edge)], 3).wait()

        @pl.when(stage == 2)
        def _():
            wait_v[top, :] = acc_v[top, :]
            hold_v[pl.ds(edge, edge), :] = low_v[pl.ds(end, edge), :]
            puts = [
                put(low_v.at[pl.ds(half, mid - half)], go_right.at[pl.ds(half, mid - half)], 2),
                put(low_v.at[pl.ds(mid, late)], go_right_late, 3),
            ]
            for copy in puts:
                copy.wait()

    for i in order:
        far_piece(i).start()
    for i in range(2):
        held_piece(i).start()

    @pl.loop(0, chips)
    def _(stage):
        span = pl.ds(pl.multiple_of(chip_of(stage) * CORES * rows, 16), CORES * rows)
        load_pre = pltpu.make_async_copy(pre.at[span], pre_v, load_sem.at[0])
        load = pltpu.make_async_copy(dyg.at[span], dy_v, load_sem.at[1])
        load_pre.start()
        load.start()
        load_pre.wait()

        @pl.loop(0, cols // tile)
        def _(m):
            ms = pl.ds(pl.multiple_of(m * tile, tile), tile)
            pair_v[:, ms] = jnp.square(jnp.maximum(pre_v[:, ms].astype(F32), 0.0)).astype(BF16)

        load.wait()

        @pl.loop(0, cols // tile)
        def _(m):
            ms = pl.ds(pl.multiple_of(m * tile, tile), tile)

            @pl.loop(0, CORES)
            def _(t):
                wide = depth // CORES
                ns = pl.ds(pl.multiple_of(t * wide, wide), wide)
                dw_v[ms, ns] += lax.dot_general(pair_v[:, ms], dy_v[:, ns], TN, preferred_element_type=F32)

    @pl.loop(0, cols // tile)
    def _(m):
        ms = pl.ds(pl.multiple_of(m * tile, tile), tile)
        wd_v[ms, :] = dw_v[ms, :].astype(BF16)

    put_dw = put(wd_v, dw_down, 4)

    gx.arrived(R1, L0)
    gx.start(PL1, PR0)
    gx.arrived(FR, FL)
    gx.start(PO0, PO1)
    gx.arrived(OWN, PL0, PL1, PR0, PR1, PO0, PO1)
    gy.sent()
    gx.sent()

    puts = []
    for i in order:
        start, size, _, target = pieces[i]
        span = pl.ds(start, size)
        far_piece(i).wait()
        dy_v[span, :] = (wait_v[span, :] + far_v[span, :].astype(F32)).astype(BF16)
        puts.append(put(dy_v.at[span], target, (0, 1, 2, 3, 5)[i]))
    for copy in puts:
        copy.wait()
    put_dw.wait()
    for i in range(2):
        held_piece(i).wait()


def solution(mesh):
    n = mesh.shape["tp"]
    chips = n // CORES

    def gather(x, dy, pre, w_in, w_down):
        rows, depth = x.shape
        tokens, cols = pre.shape
        early = rows - EDGE - LATE
        anywhere = pl.BlockSpec(memory_space=pl.ANY)
        shape = jax.ShapeDtypeStruct
        return pl.pallas_call(
            functools.partial(gather_kernel, chips),
            name="gather",
            out_shape=(
                shape((tokens, depth), BF16),
                shape((tokens, depth), BF16),
                shape((tokens, cols), BF16),
                shape((rows - LATE, depth), F32),
                shape((LATE, depth), F32),
                shape((early, depth), BF16),
                shape((LATE, depth), BF16),
                shape((early, depth), BF16),
                shape((LATE, depth), BF16),
                shape((EDGE, depth), BF16),
                shape((EDGE, depth), BF16),
                shape((cols, depth), BF16),
            ),
            in_specs=[anywhere] * 5,
            out_specs=(anywhere,) * 12,
            scratch_shapes=[
                pltpu.VMEM((cols, depth), BF16),
                pltpu.VMEM((depth, cols), BF16),
                pltpu.VMEM((depth, cols), BF16),
                pltpu.VMEM((CORES * rows, depth), BF16),
                pltpu.VMEM((CORES * rows, cols), BF16),
                pltpu.VMEM((CORES * rows, cols), BF16),
                pltpu.VMEM((chips, rows, cols), BF16),
                pltpu.VMEM((rows, depth), F32),
                pltpu.VMEM((rows, depth), BF16),
                pltpu.VMEM((rows, depth), F32),
                pltpu.VMEM((rows, depth), BF16),
                pltpu.VMEM((2 * EDGE, depth), BF16),
                pltpu.VMEM((cols, depth), F32),
                pltpu.SemaphoreType.DMA((2, COPIES)),
                pltpu.SemaphoreType.DMA((2, COPIES)),
                pltpu.SemaphoreType.DMA,
                pltpu.SemaphoreType.DMA((chips,)),
                pltpu.SemaphoreType.DMA,
                pltpu.SemaphoreType.DMA,
                pltpu.SemaphoreType.DMA((5,)),
                pltpu.SemaphoreType.DMA((5,)),
                pltpu.SemaphoreType.DMA((2,)),
                pltpu.SemaphoreType.DMA((2,)),
                pltpu.SemaphoreType.DMA((4,)),
                pltpu.SemaphoreType.DMA((6,)),
            ],
            compiler_params=pltpu.CompilerParams(
                collective_id=0, has_side_effects=True, vmem_limit_bytes=64 * 1024 * 1024 - 65536
            ),
            cost_estimate=pl.CostEstimate(
                flops=6 * tokens * depth * cols, bytes_accessed=8 * tokens * depth, transcendentals=0
            ),
        )(x, dy, pre, w_in, w_down)

    def weight_grad(xg, d_pre, done, tile=384):
        tokens, depth = xg.shape
        cols = d_pre.shape[1]
        steps = depth // tile

        def body(x_ref, d_ref, done_ref, out_ref, copy_ref):
            copy_ref[...] = done_ref[...]
            out_ref[...] = lax.dot_general(x_ref[...], d_ref[...], TN, preferred_element_type=F32).astype(BF16)

        side = pl.BlockSpec((done.shape[0] // steps, done.shape[1]), lambda i: (i, 0))
        return pl.pallas_call(
            body, name="weight_grad", grid=(steps,),
            in_specs=[pl.BlockSpec((tokens, tile), lambda i: (0, i)), pl.BlockSpec((tokens, cols), lambda i: (0, 0)), side],
            out_specs=(pl.BlockSpec((tile, cols), lambda i: (i, 0)), side),
            out_shape=(jax.ShapeDtypeStruct((depth, cols), BF16), jax.ShapeDtypeStruct(done.shape, done.dtype)),
            compiler_params=pltpu.CompilerParams(vmem_limit_bytes=62 * 1024 * 1024),
            cost_estimate=pl.CostEstimate(
                flops=2 * tokens * depth * cols, bytes_accessed=2 * tokens * (depth + cols) + 6 * depth * cols, transcendentals=0
            ),
        )(xg, d_pre, done)

    def step(x, dy, pre, w_in, w_down):
        clockwise = [(i, (i + CORES) % n) for i in range(n)]
        counter = [(i, (i - CORES) % n) for i in range(n)]
        (
            xg, _, d_pre, s_own, s_own_late, go_left, go_left_late, go_right, go_right_late, got_left, got_right, dw_down
        ) = gather(x, dy, pre, w_in, w_down)
        from_left = lax.ppermute(go_right, "tp", clockwise)
        from_right = lax.ppermute(go_left, "tp", counter)
        from_left_late = lax.ppermute(go_right_late, "tp", clockwise)
        from_right_late = lax.ppermute(go_left_late, "tp", counter)
        dw_in, dw_down = weight_grad(xg, d_pre, dw_down)
        s_own, dw_in, dw_down = lax.optimization_barrier((s_own, dw_in, dw_down))
        mid = go_right.shape[0]
        one, other, top, bottom = (t.astype(F32) for t in (from_left, from_right, got_right, got_left))
        dx = jnp.concatenate([
            s_own[:EDGE] + one[:EDGE] + top,
            s_own[EDGE:mid] + one[EDGE:] + other[:mid - EDGE],
            jnp.zeros_like(s_own_late),
            s_own[mid:] + bottom + other[mid - EDGE:],
        ]).astype(BF16)
        dx = lax.optimization_barrier(dx)
        late = s_own_late + from_left_late.astype(F32) + from_right_late.astype(F32)
        dx = lax.dynamic_update_slice(dx, late.astype(BF16), (mid, 0))
        return dx, dw_in, dw_down

    tokens, columns, weight_rows = P(("dp", "tp"), None), P(None, "tp"), P("tp", None)
    return jax.shard_map(
        step,
        mesh=mesh,
        in_specs=(tokens, tokens, P("dp", "tp"), columns, weight_rows),
        out_specs=(tokens, P("dp", "tp"), P(("dp", "tp"), None)),
        check_vma=False,
    )
```

```python
import functools

import jax
import jax.numpy as jnp
from jax import lax
from jax.experimental import pallas as pl
from jax.experimental.pallas import tpu as pltpu
from jax.sharding import PartitionSpec as P


CORES = 2
LATE, EDGE = 64, 32
F32, BF16 = jnp.float32, jnp.bfloat16
NT = (((1,), (1,)), ((), ()))
TN = (((0,), (0,)), ((), ()))

(R0, R1, L0, L1, OWN, FR, FL, PL0, PL1, PR0, PR1, PO0, PO1) = range(13)
COPIES = 13


def gather_kernel(
    chips, x, dy, pre, w_in, w_down,
    xg, dyg, d_pre, s_own, s_own_late, go_left, go_left_late, go_right, go_right_late, got_left, got_right, dw_down,
    wd_v, wi_v, wp_v, dy_v, pre_v, pair_v, got_v, acc_v, low_v, wait_v, far_v, hold_v, dw_v,
    send_sem, recv_sem, got_send, got_recv, w_send, w_recv, far_send, far_recv, hold_send, hold_recv, load_sem, store_sem,
):
    rows, depth = dy.shape
    half = rows // 2
    cols = w_down.shape[0]
    tile = 384
    first, top, bottom = pl.ds(0, rows), pl.ds(0, half), pl.ds(half, half)
    mine_v, other_v = pair_v.at[first], pair_v.at[pl.ds(rows, rows)]
    me = lax.axis_index("tp")
    chip, core = me // CORES, lax.rem(me, CORES)
    left = lax.rem(chip + chips - 1, chips)
    right = lax.rem(chip + 1, chips)
    far = lax.rem(chip + 2, chips)

    def device(c, k):
        return {"tp": c * CORES + k}

    to_right, to_left, to_partner = device(right, core), device(left, core), device(chip, 1 - core)

    def block(ref, c, k, h=None):
        start = (c * CORES + k) * rows
        if h is None:
            return ref.at[pl.ds(pl.multiple_of(start, 16), rows)]
        return ref.at[pl.ds(pl.multiple_of(start + h * half, 16), half)]

    class Gather:
        def __init__(self, which, src, dst):
            self.which, self.src, self.dst = which, src, dst

        def own(self, h):
            return self.src.at[pl.ds(h * half, half)]

        def copy(self, n, src, dst, target):
            return pltpu.make_async_remote_copy(
                src_ref=src, dst_ref=dst, send_sem=send_sem.at[self.which, n], recv_sem=recv_sem.at[self.which, n],
                device_id=target, device_id_type=pl.DeviceIdType.MESH,
            )

        def out(self, n):
            d = self.dst
            if n in (R0, R1):
                h = n - R0
                return self.copy(n, self.own(h), block(d, chip, core, h), to_right)
            if n in (L0, L1):
                h = n - L0
                return self.copy(n, self.own(h), block(d, chip, core, h), to_left)
            if n == OWN:
                return self.copy(n, self.src, block(d, chip, core), to_partner)
            if n == FR:
                return self.copy(n, block(d, left, core, 0), block(d, left, core, 0), to_right)
            if n == FL:
                return self.copy(n, block(d, right, core, 1), block(d, right, core, 1), to_left)
            c, h = {PL0: (left, 0), PL1: (left, 1), PR0: (right, 0), PR1: (right, 1), PO0: (far, 0), PO1: (far, 1)}[n]
            return self.copy(n, block(d, c, core, h), block(d, c, core, h), to_partner)

        def start(self, *names):
            for n in names:
                self.out(n).start()

        def arrived(self, *names):
            for n in names:
                if n == OWN:
                    dst = block(self.dst, chip, 1 - core)
                else:
                    c, k, h = {
                        R0: (left, core, 0), R1: (left, core, 1), L0: (right, core, 0), L1: (right, core, 1),
                        FR: (far, core, 0), FL: (far, core, 1),
                        PL0: (left, 1 - core, 0), PL1: (left, 1 - core, 1), PR0: (right, 1 - core, 0),
                        PR1: (right, 1 - core, 1), PO0: (far, 1 - core, 0), PO1: (far, 1 - core, 1),
                    }[n]
                    dst = block(self.dst, c, k, h)
                self.copy(n, dst, dst, to_partner).wait_recv()

        def sent(self):
            for n in range(COPIES):
                self.out(n).wait_send()

    gy, gx = Gather(0, dy, dyg), Gather(1, x, xg)

    barrier = pltpu.get_barrier_semaphore()
    for target in (to_right, to_left, to_partner):
        pl.semaphore_signal(barrier, inc=1, device_id=target, device_id_type=pl.DeviceIdType.MESH)
    load_wd = pltpu.make_async_copy(w_down, wd_v, load_sem.at[0])
    load_dy = pltpu.make_async_copy(dy, dy_v.at[first], load_sem.at[1])
    load_x = pltpu.make_async_copy(x, low_v, load_sem.at[2])
    load_wi = pltpu.make_async_copy(w_in, wi_v, load_sem.at[3])
    load_dy.start()
    load_wd.start()
    pl.semaphore_wait(barrier, 3)

    gy.start(R0, L1, OWN, R1, L0)
    gx.start(R0, L1)
    load_x.start()
    load_wi.start()
    give_w = pltpu.make_async_remote_copy(
        src_ref=w_in, dst_ref=wp_v, send_sem=w_send, recv_sem=w_recv,
        device_id=to_partner, device_id_type=pl.DeviceIdType.MESH,
    )
    give_w.start()

    load_dy.wait()
    keep_dy = pltpu.make_async_copy(dy_v.at[first], block(dyg, chip, core), store_sem.at[0])
    keep_dy.start()
    load_x.wait()
    keep_x = pltpu.make_async_copy(low_v, block(xg, chip, core), store_sem.at[1])
    keep_x.start()
    load_wd.wait()
    load_wi.wait()

    def chip_of(stage):
        return lax.rem(chip + jnp.where(stage == 0, 0, jnp.where(stage == 1, chips - 1, stage - 1)), chips)

    def hidden_grad(stage, k, out_v):
        c = chip_of(stage)
        load_pre = pltpu.make_async_copy(block(pre, c, k), pre_v.at[first], load_sem.at[0])
        load_pre.start()
        load = pltpu.make_async_copy(block(dyg, c, k), dy_v.at[first], load_sem.at[1])
        load.start()
        load.wait()
        load_pre.wait()

        @pl.loop(0, cols // tile)
        def _(t):
            span = pl.ds(pl.multiple_of(t * tile, tile), tile)
            grad = lax.dot_general(dy_v[first, :], wd_v[span, :], NT, preferred_element_type=F32)
            p = pre_v[first, span].astype(F32)
            out_v[:, span] = jnp.where(p > 0, grad * (2.0 * p), 0.0).astype(BF16)

        keep = pltpu.make_async_copy(out_v, block(d_pre, c, k), store_sem.at[2])
        keep.start()
        return keep

    def swap(stage):
        return pltpu.make_async_remote_copy(
            src_ref=other_v, dst_ref=got_v.at[stage], send_sem=got_send, recv_sem=got_recv.at[stage],
            device_id=to_partner, device_id_type=pl.DeviceIdType.MESH,
        )

    keep_dy.wait()
    keep_x.wait()
    dw_v[...] = jnp.zeros_like(dw_v)

    edge, late = got_left.shape[0], go_left_late.shape[0]
    mid, end = rows - edge - late, rows - edge
    cut = half // 32 * 16
    pieces = [
        (0, cut, to_right, go_right.at[pl.ds(0, cut)]),
        (cut, half - cut, to_right, go_right.at[pl.ds(cut, half - cut)]),
        (half, mid - half, to_left, go_left.at[pl.ds(half - edge, mid - half)]),
        (mid, late, to_left, go_left_late),
        (end, edge, to_left, go_left.at[pl.ds(mid - edge, edge)]),
    ]
    order = (0, 2, 1, 3, 4)

    def far_piece(i):
        start, size, target, _ = pieces[i]
        span = pl.ds(start, size)
        return pltpu.make_async_remote_copy(
            src_ref=low_v.at[span], dst_ref=far_v.at[span], send_sem=far_send.at[i], recv_sem=far_recv.at[i],
            device_id=target, device_id_type=pl.DeviceIdType.MESH,
        )

    def held_piece(i):
        return pltpu.make_async_remote_copy(
            src_ref=hold_v.at[pl.ds(i * edge, edge)], dst_ref=(got_right, got_left)[i],
            send_sem=hold_send.at[i], recv_sem=hold_recv.at[i],
            device_id=(to_left, to_right)[i], device_id_type=pl.DeviceIdType.MESH,
        )

    def put(src, dst, i):
        copy = pltpu.make_async_copy(src, dst, store_sem.at[i])
        copy.start()
        return copy

    @pl.loop(0, chips)
    def _(stage):
        @pl.when(stage == 1)
        def _():
            gy.arrived(R0, L1)
            gy.start(FR, FL, PL0, PR1)
            gx.start(R1, L0, OWN)
            gy.arrived(R1, L0)
            gy.start(PL1, PR0)

        @pl.when(stage == 3)
        def _():
            gx.arrived(R0, L1)
            gx.start(FR, FL, PL0, PR1)
            gy.arrived(FR, FL)
            gy.start(PO0, PO1)

        hidden_grad(stage, core, mine_v).wait()

        @pl.when(stage == 0)
        def _():
            gy.arrived(OWN)

        @pl.when(stage == 1)
        def _():
            gy.arrived(PL0, PL1)

        @pl.when(stage == 2)
        def _():
            gy.arrived(PR0, PR1)

        @pl.when(stage == 3)
        def _():
            gy.arrived(PO0, PO1)

        keep = hidden_grad(stage, 1 - core, other_v)
        give = swap(stage)
        give.start()

        @pl.when(stage == 0)
        def _():
            give_w.wait()

        give.wait_recv()
        wide = 512

        @pl.loop(0, depth // wide)
        def _(t):
            span = pl.ds(pl.multiple_of(t * wide, wide), wide)
            term = lax.dot_general(mine_v[...], wi_v[span, :], NT, preferred_element_type=F32)
            term += lax.dot_general(got_v[stage], wp_v[span, :], NT, preferred_element_type=F32)
            acc_v[:, span] = term
            low_v[:, span] = term.astype(BF16)

        give.wait_send()
        keep.wait()

        @pl.when(stage == 0)
        def _():
            puts = [
                put(acc_v.at[pl.ds(0, mid)], s_own.at[pl.ds(0, mid)], 1),
                put(acc_v.at[pl.ds(mid, late)], s_own_late, 2),
                put(acc_v.at[pl.ds(end, edge)], s_own.at[pl.ds(mid, edge)], 3),
            ]
            for copy in puts:
                copy.wait()

        @pl.when(stage == 1)
        def _():
            wait_v[bottom, :] = acc_v[bottom, :]
            hold_v[pl.ds(0, edge), :] = low_v[pl.ds(0, edge), :]
            put(low_v.at[pl.ds(edge, half - edge)], go_left.at[pl.ds(0, half - edge)], 3).wait()

        @pl.when(stage == 2)
        def _():
            wait_v[top, :] = acc_v[top, :]
            hold_v[pl.ds(edge, edge), :] = low_v[pl.ds(end, edge), :]
            puts = [
                put(low_v.at[pl.ds(half, mid - half)], go_right.at[pl.ds(half, mid - half)], 2),
                put(low_v.at[pl.ds(mid, late)], go_right_late, 3),
            ]
            for copy in puts:
                copy.wait()

    for i in order:
        far_piece(i).start()
    for i in range(2):
        held_piece(i).start()

    @pl.loop(0, chips)
    def _(stage):
        span = pl.ds(pl.multiple_of(chip_of(stage) * CORES * rows, 16), CORES * rows)
        load_pre = pltpu.make_async_copy(pre.at[span], pre_v, load_sem.at[0])
        load = pltpu.make_async_copy(dyg.at[span], dy_v, load_sem.at[1])
        load_pre.start()
        load.start()
        load_pre.wait()

        @pl.loop(0, cols // tile)
        def _(m):
            ms = pl.ds(pl.multiple_of(m * tile, tile), tile)
            pair_v[:, ms] = jnp.square(jnp.maximum(pre_v[:, ms].astype(F32), 0.0)).astype(BF16)

        load.wait()

        @pl.loop(0, cols // tile)
        def _(m):
            ms = pl.ds(pl.multiple_of(m * tile, tile), tile)

            @pl.loop(0, CORES)
            def _(t):
                wide = depth // CORES
                ns = pl.ds(pl.multiple_of(t * wide, wide), wide)
                dw_v[ms, ns] += lax.dot_general(pair_v[:, ms], dy_v[:, ns], TN, preferred_element_type=F32)

    @pl.loop(0, cols // tile)
    def _(m):
        ms = pl.ds(pl.multiple_of(m * tile, tile), tile)
        wd_v[ms, :] = dw_v[ms, :].astype(BF16)

    put_dw = put(wd_v, dw_down, 4)

    gx.arrived(R1, L0)
    gx.start(PL1, PR0)
    gx.arrived(FR, FL)
    gx.start(PO0, PO1)
    gx.arrived(OWN, PL0, PL1, PR0, PR1, PO0, PO1)
    gy.sent()
    gx.sent()

    puts = []
    for i in order:
        start, size, _, target = pieces[i]
        span = pl.ds(start, size)
        far_piece(i).wait()
        dy_v[span, :] = (wait_v[span, :] + far_v[span, :].astype(F32)).astype(BF16)
        puts.append(put(dy_v.at[span], target, (0, 1, 2, 3, 5)[i]))
    for copy in puts:
        copy.wait()
    put_dw.wait()
    for i in range(2):
        held_piece(i).wait()


def solution(mesh):
    n = mesh.shape["tp"]
    chips = n // CORES

    def gather(x, dy, pre, w_in, w_down):
        rows, depth = x.shape
        tokens, cols = pre.shape
        early = rows - EDGE - LATE
        anywhere = pl.BlockSpec(memory_space=pl.ANY)
        shape = jax.ShapeDtypeStruct
        return pl.pallas_call(
            functools.partial(gather_kernel, chips),
            name="gather",
            out_shape=(
                shape((tokens, depth), BF16),
                shape((tokens, depth), BF16),
                shape((tokens, cols), BF16),
                shape((rows - LATE, depth), F32),
                shape((LATE, depth), F32),
                shape((early, depth), BF16),
                shape((LATE, depth), BF16),
                shape((early, depth), BF16),
                shape((LATE, depth), BF16),
                shape((EDGE, depth), BF16),
                shape((EDGE, depth), BF16),
                shape((cols, depth), BF16),
            ),
            in_specs=[anywhere] * 5,
            out_specs=(anywhere,) * 12,
            scratch_shapes=[
                pltpu.VMEM((cols, depth), BF16),
                pltpu.VMEM((depth, cols), BF16),
                pltpu.VMEM((depth, cols), BF16),
                pltpu.VMEM((CORES * rows, depth), BF16),
                pltpu.VMEM((CORES * rows, cols), BF16),
                pltpu.VMEM((CORES * rows, cols), BF16),
                pltpu.VMEM((chips, rows, cols), BF16),
                pltpu.VMEM((rows, depth), F32),
                pltpu.VMEM((rows, depth), BF16),
                pltpu.VMEM((rows, depth), F32),
                pltpu.VMEM((rows, depth), BF16),
                pltpu.VMEM((2 * EDGE, depth), BF16),
                pltpu.VMEM((cols, depth), F32),
                pltpu.SemaphoreType.DMA((2, COPIES)),
                pltpu.SemaphoreType.DMA((2, COPIES)),
                pltpu.SemaphoreType.DMA,
                pltpu.SemaphoreType.DMA((chips,)),
                pltpu.SemaphoreType.DMA,
                pltpu.SemaphoreType.DMA,
                pltpu.SemaphoreType.DMA((5,)),
                pltpu.SemaphoreType.DMA((5,)),
                pltpu.SemaphoreType.DMA((2,)),
                pltpu.SemaphoreType.DMA((2,)),
                pltpu.SemaphoreType.DMA((4,)),
                pltpu.SemaphoreType.DMA((6,)),
            ],
            compiler_params=pltpu.CompilerParams(
                collective_id=0, has_side_effects=True, vmem_limit_bytes=64 * 1024 * 1024 - 65536
            ),
            cost_estimate=pl.CostEstimate(
                flops=6 * tokens * depth * cols, bytes_accessed=8 * tokens * depth, transcendentals=0
            ),
        )(x, dy, pre, w_in, w_down)

    def weight_grad(xg, d_pre, done, tile=384):
        tokens, depth = xg.shape
        cols = d_pre.shape[1]
        steps = depth // tile

        def body(x_ref, d_ref, done_ref, out_ref, copy_ref):
            copy_ref[...] = done_ref[...]
            out_ref[...] = lax.dot_general(x_ref[...], d_ref[...], TN, preferred_element_type=F32).astype(BF16)

        side = pl.BlockSpec((done.shape[0] // steps, done.shape[1]), lambda i: (i, 0))
        return pl.pallas_call(
            body, name="weight_grad", grid=(steps,),
            in_specs=[pl.BlockSpec((tokens, tile), lambda i: (0, i)), pl.BlockSpec((tokens, cols), lambda i: (0, 0)), side],
            out_specs=(pl.BlockSpec((tile, cols), lambda i: (i, 0)), side),
            out_shape=(jax.ShapeDtypeStruct((depth, cols), BF16), jax.ShapeDtypeStruct(done.shape, done.dtype)),
            compiler_params=pltpu.CompilerParams(vmem_limit_bytes=62 * 1024 * 1024),
            cost_estimate=pl.CostEstimate(
                flops=2 * tokens * depth * cols, bytes_accessed=2 * tokens * (depth + cols) + 6 * depth * cols, transcendentals=0
            ),
        )(xg, d_pre, done)

    def keep_in_hbm(a):
        anywhere = pl.BlockSpec(memory_space=pl.ANY)
        return pl.pallas_call(
            lambda a_ref, out_ref: None, name="keep_in_hbm", in_specs=[anywhere], out_specs=anywhere,
            out_shape=jax.ShapeDtypeStruct(a.shape, a.dtype), input_output_aliases={0: 0},
        )(a)

    def step(x, dy, pre, w_in, w_down):
        clockwise = [(i, (i + CORES) % n) for i in range(n)]
        counter = [(i, (i - CORES) % n) for i in range(n)]
        (
            xg, _, d_pre, s_own, s_own_late, go_left, go_left_late, go_right, go_right_late, got_left, got_right, dw_down
        ) = gather(x, dy, pre, w_in, w_down)
        from_left = lax.ppermute(go_right, "tp", clockwise)
        from_right = lax.ppermute(go_left, "tp", counter)
        from_left_late = lax.ppermute(go_right_late, "tp", clockwise)
        from_right_late = lax.ppermute(go_left_late, "tp", counter)
        dw_in, dw_down = weight_grad(xg, d_pre, dw_down)
        s_own, dw_in, dw_down = lax.optimization_barrier((s_own, dw_in, dw_down))
        mid = go_right.shape[0]
        one, other, top, bottom = (t.astype(F32) for t in (from_left, from_right, got_right, got_left))
        dx = jnp.concatenate([
            s_own[:EDGE] + one[:EDGE] + top,
            s_own[EDGE:mid] + one[EDGE:] + other[:mid - EDGE],
            jnp.zeros_like(s_own_late),
            s_own[mid:] + bottom + other[mid - EDGE:],
        ]).astype(BF16)
        dx = keep_in_hbm(dx)
        late = s_own_late + from_left_late.astype(F32) + from_right_late.astype(F32)
        dx = lax.dynamic_update_slice(dx, late.astype(BF16), (mid, 0))
        return dx, dw_in, dw_down

    tokens, columns, weight_rows = P(("dp", "tp"), None), P(None, "tp"), P("tp", None)
    return jax.shard_map(
        step,
        mesh=mesh,
        in_specs=(tokens, tokens, P("dp", "tp"), columns, weight_rows),
        out_specs=(tokens, P("dp", "tp"), P(("dp", "tp"), None)),
        check_vma=False,
    )
```

```python
import functools

import jax
import jax.numpy as jnp
from jax import lax
from jax.experimental import pallas as pl
from jax.experimental.pallas import tpu as pltpu
from jax.sharding import PartitionSpec as P


CORES = 2
LATE, EDGE = 32, 32
F32, BF16 = jnp.float32, jnp.bfloat16
NT = (((1,), (1,)), ((), ()))
TN = (((0,), (0,)), ((), ()))

(R0, R1, L0, L1, OWN, FR, FL, PL0, PL1, PR0, PR1, PO0, PO1) = range(13)
COPIES = 13


def gather_kernel(
    chips, x, dy, pre, w_in, w_down,
    xg, dyg, d_pre, s_own, go_left, go_left_late, go_right, go_right_late, got_left, got_right, dw_down,
    wd_v, wi_v, wp_v, dy_v, pre_v, pair_v, got_v, acc_v, low_v, wait_v, far_v, hold_v, dw_v,
    send_sem, recv_sem, got_send, got_recv, w_send, w_recv, far_send, far_recv, hold_send, hold_recv, load_sem, store_sem,
):
    rows, depth = dy.shape
    half = rows // 2
    cols = w_down.shape[0]
    tile = 384
    first, top, bottom = pl.ds(0, rows), pl.ds(0, half), pl.ds(half, half)
    mine_v, other_v = pair_v.at[first], pair_v.at[pl.ds(rows, rows)]
    me = lax.axis_index("tp")
    chip, core = me // CORES, lax.rem(me, CORES)
    left = lax.rem(chip + chips - 1, chips)
    right = lax.rem(chip + 1, chips)
    far = lax.rem(chip + 2, chips)

    def device(c, k):
        return {"tp": c * CORES + k}

    to_right, to_left, to_partner = device(right, core), device(left, core), device(chip, 1 - core)

    def block(ref, c, k, h=None):
        start = (c * CORES + k) * rows
        if h is None:
            return ref.at[pl.ds(pl.multiple_of(start, 16), rows)]
        return ref.at[pl.ds(pl.multiple_of(start + h * half, 16), half)]

    class Gather:
        def __init__(self, which, src, dst):
            self.which, self.src, self.dst = which, src, dst

        def own(self, h):
            return self.src.at[pl.ds(h * half, half)]

        def copy(self, n, src, dst, target):
            return pltpu.make_async_remote_copy(
                src_ref=src, dst_ref=dst, send_sem=send_sem.at[self.which, n], recv_sem=recv_sem.at[self.which, n],
                device_id=target, device_id_type=pl.DeviceIdType.MESH,
            )

        def out(self, n):
            d = self.dst
            if n in (R0, R1):
                h = n - R0
                return self.copy(n, self.own(h), block(d, chip, core, h), to_right)
            if n in (L0, L1):
                h = n - L0
                return self.copy(n, self.own(h), block(d, chip, core, h), to_left)
            if n == OWN:
                return self.copy(n, self.src, block(d, chip, core), to_partner)
            if n == FR:
                return self.copy(n, block(d, left, core, 0), block(d, left, core, 0), to_right)
            if n == FL:
                return self.copy(n, block(d, right, core, 1), block(d, right, core, 1), to_left)
            c, h = {PL0: (left, 0), PL1: (left, 1), PR0: (right, 0), PR1: (right, 1), PO0: (far, 0), PO1: (far, 1)}[n]
            return self.copy(n, block(d, c, core, h), block(d, c, core, h), to_partner)

        def start(self, *names):
            for n in names:
                self.out(n).start()

        def arrived(self, *names):
            for n in names:
                if n == OWN:
                    dst = block(self.dst, chip, 1 - core)
                else:
                    c, k, h = {
                        R0: (left, core, 0), R1: (left, core, 1), L0: (right, core, 0), L1: (right, core, 1),
                        FR: (far, core, 0), FL: (far, core, 1),
                        PL0: (left, 1 - core, 0), PL1: (left, 1 - core, 1), PR0: (right, 1 - core, 0),
                        PR1: (right, 1 - core, 1), PO0: (far, 1 - core, 0), PO1: (far, 1 - core, 1),
                    }[n]
                    dst = block(self.dst, c, k, h)
                self.copy(n, dst, dst, to_partner).wait_recv()

        def sent(self):
            for n in range(COPIES):
                self.out(n).wait_send()

    gy, gx = Gather(0, dy, dyg), Gather(1, x, xg)

    barrier = pltpu.get_barrier_semaphore()
    for target in (to_right, to_left, to_partner):
        pl.semaphore_signal(barrier, inc=1, device_id=target, device_id_type=pl.DeviceIdType.MESH)
    load_wd = pltpu.make_async_copy(w_down, wd_v, load_sem.at[0])
    load_dy = pltpu.make_async_copy(dy, dy_v.at[first], load_sem.at[1])
    load_x = pltpu.make_async_copy(x, low_v, load_sem.at[2])
    load_wi = pltpu.make_async_copy(w_in, wi_v, load_sem.at[3])
    load_dy.start()
    load_wd.start()
    pl.semaphore_wait(barrier, 3)

    gy.start(R0, L1, OWN, R1, L0)
    gx.start(R0, L1)
    load_x.start()
    load_wi.start()
    give_w = pltpu.make_async_remote_copy(
        src_ref=w_in, dst_ref=wp_v, send_sem=w_send, recv_sem=w_recv,
        device_id=to_partner, device_id_type=pl.DeviceIdType.MESH,
    )
    give_w.start()

    load_dy.wait()
    keep_dy = pltpu.make_async_copy(dy_v.at[first], block(dyg, chip, core), store_sem.at[0])
    keep_dy.start()
    load_x.wait()
    keep_x = pltpu.make_async_copy(low_v, block(xg, chip, core), store_sem.at[1])
    keep_x.start()
    load_wd.wait()
    load_wi.wait()

    def chip_of(stage):
        return lax.rem(chip + jnp.where(stage == 0, 0, jnp.where(stage == 1, chips - 1, stage - 1)), chips)

    def hidden_grad(stage, k, out_v):
        c = chip_of(stage)
        load_pre = pltpu.make_async_copy(block(pre, c, k), pre_v.at[first], load_sem.at[0])
        load_pre.start()
        load = pltpu.make_async_copy(block(dyg, c, k), dy_v.at[first], load_sem.at[1])
        load.start()
        load.wait()
        load_pre.wait()

        @pl.loop(0, cols // tile)
        def _(t):
            span = pl.ds(pl.multiple_of(t * tile, tile), tile)
            grad = lax.dot_general(dy_v[first, :], wd_v[span, :], NT, preferred_element_type=F32)
            p = pre_v[first, span].astype(F32)
            out_v[:, span] = jnp.where(p > 0, grad * (2.0 * p), 0.0).astype(BF16)

        keep = pltpu.make_async_copy(out_v, block(d_pre, c, k), store_sem.at[2])
        keep.start()
        return keep

    def swap(stage):
        return pltpu.make_async_remote_copy(
            src_ref=other_v, dst_ref=got_v.at[stage], send_sem=got_send, recv_sem=got_recv.at[stage],
            device_id=to_partner, device_id_type=pl.DeviceIdType.MESH,
        )

    keep_dy.wait()
    keep_x.wait()
    dw_v[...] = jnp.zeros_like(dw_v)

    edge, late = got_left.shape[0], go_left_late.shape[0]
    mid, end = rows - edge - late, rows - edge
    cut = half // 32 * 16
    pieces = [
        (0, cut, to_right, go_right.at[pl.ds(0, cut)]),
        (cut, half - cut, to_right, go_right.at[pl.ds(cut, half - cut)]),
        (half, mid - half, to_left, go_left.at[pl.ds(half - edge, mid - half)]),
        (mid, late, to_left, go_left_late),
        (end, edge, to_left, go_left.at[pl.ds(mid - edge, edge)]),
    ]
    order = (0, 2, 1, 3, 4)

    def far_piece(i):
        start, size, target, _ = pieces[i]
        span = pl.ds(start, size)
        return pltpu.make_async_remote_copy(
            src_ref=low_v.at[span], dst_ref=far_v.at[span], send_sem=far_send.at[i], recv_sem=far_recv.at[i],
            device_id=target, device_id_type=pl.DeviceIdType.MESH,
        )

    def held_piece(i):
        return pltpu.make_async_remote_copy(
            src_ref=hold_v.at[pl.ds(i * edge, edge)], dst_ref=(got_right, got_left)[i],
            send_sem=hold_send.at[i], recv_sem=hold_recv.at[i],
            device_id=(to_left, to_right)[i], device_id_type=pl.DeviceIdType.MESH,
        )

    def put(src, dst, i):
        copy = pltpu.make_async_copy(src, dst, store_sem.at[i])
        copy.start()
        return copy

    @pl.loop(0, chips)
    def _(stage):
        @pl.when(stage == 1)
        def _():
            gy.arrived(R0, L1)
            gy.start(FR, FL, PL0, PR1)
            gx.start(R1, L0, OWN)
            gy.arrived(R1, L0)
            gy.start(PL1, PR0)

        @pl.when(stage == 3)
        def _():
            gx.arrived(R0, L1)
            gx.start(FR, FL, PL0, PR1)
            gy.arrived(FR, FL)
            gy.start(PO0, PO1)

        hidden_grad(stage, core, mine_v).wait()

        @pl.when(stage == 0)
        def _():
            gy.arrived(OWN)

        @pl.when(stage == 1)
        def _():
            gy.arrived(PL0, PL1)

        @pl.when(stage == 2)
        def _():
            gy.arrived(PR0, PR1)

        @pl.when(stage == 3)
        def _():
            gy.arrived(PO0, PO1)

        keep = hidden_grad(stage, 1 - core, other_v)
        give = swap(stage)
        give.start()

        @pl.when(stage == 0)
        def _():
            give_w.wait()

        give.wait_recv()
        wide = 512

        @pl.loop(0, depth // wide)
        def _(t):
            span = pl.ds(pl.multiple_of(t * wide, wide), wide)
            term = lax.dot_general(mine_v[...], wi_v[span, :], NT, preferred_element_type=F32)
            term += lax.dot_general(got_v[stage], wp_v[span, :], NT, preferred_element_type=F32)
            acc_v[:, span] = term
            low_v[:, span] = term.astype(BF16)

        give.wait_send()
        keep.wait()

        @pl.when(stage == 0)
        def _():
            put(acc_v, s_own, 3).wait()

        @pl.when(stage == 1)
        def _():
            wait_v[bottom, :] = acc_v[bottom, :]
            hold_v[pl.ds(0, edge), :] = low_v[pl.ds(0, edge), :]
            put(low_v.at[pl.ds(edge, half - edge)], go_left.at[pl.ds(0, half - edge)], 3).wait()

        @pl.when(stage == 2)
        def _():
            wait_v[top, :] = acc_v[top, :]
            hold_v[pl.ds(edge, edge), :] = low_v[pl.ds(end, edge), :]
            puts = [
                put(low_v.at[pl.ds(half, mid - half)], go_right.at[pl.ds(half, mid - half)], 2),
                put(low_v.at[pl.ds(mid, late)], go_right_late, 3),
            ]
            for copy in puts:
                copy.wait()

    for i in order:
        far_piece(i).start()
    for i in range(2):
        held_piece(i).start()

    @pl.loop(0, chips)
    def _(stage):
        span = pl.ds(pl.multiple_of(chip_of(stage) * CORES * rows, 16), CORES * rows)
        load_pre = pltpu.make_async_copy(pre.at[span], pre_v, load_sem.at[0])
        load = pltpu.make_async_copy(dyg.at[span], dy_v, load_sem.at[1])
        load_pre.start()
        load.start()
        load_pre.wait()

        @pl.loop(0, cols // tile)
        def _(m):
            ms = pl.ds(pl.multiple_of(m * tile, tile), tile)
            pair_v[:, ms] = jnp.square(jnp.maximum(pre_v[:, ms].astype(F32), 0.0)).astype(BF16)

        load.wait()

        @pl.loop(0, cols // tile)
        def _(m):
            ms = pl.ds(pl.multiple_of(m * tile, tile), tile)

            @pl.loop(0, CORES)
            def _(t):
                wide = depth // CORES
                ns = pl.ds(pl.multiple_of(t * wide, wide), wide)
                dw_v[ms, ns] += lax.dot_general(pair_v[:, ms], dy_v[:, ns], TN, preferred_element_type=F32)

    @pl.loop(0, cols // tile)
    def _(m):
        ms = pl.ds(pl.multiple_of(m * tile, tile), tile)
        wd_v[ms, :] = dw_v[ms, :].astype(BF16)

    put_dw = put(wd_v, dw_down, 4)

    gx.arrived(R1, L0)
    gx.start(PL1, PR0)
    gx.arrived(FR, FL)
    gx.start(PO0, PO1)
    gx.arrived(OWN, PL0, PL1, PR0, PR1, PO0, PO1)
    gy.sent()
    gx.sent()

    puts = []
    for i in order:
        start, size, _, target = pieces[i]
        span = pl.ds(start, size)
        far_piece(i).wait()
        dy_v[span, :] = (wait_v[span, :] + far_v[span, :].astype(F32)).astype(BF16)
        puts.append(put(dy_v.at[span], target, (0, 1, 2, 3, 5)[i]))
    for copy in puts:
        copy.wait()
    put_dw.wait()
    for i in range(2):
        held_piece(i).wait()


def solution(mesh):
    n = mesh.shape["tp"]
    chips = n // CORES

    def gather(x, dy, pre, w_in, w_down):
        rows, depth = x.shape
        tokens, cols = pre.shape
        early = rows - EDGE - LATE
        anywhere = pl.BlockSpec(memory_space=pl.ANY)
        shape = jax.ShapeDtypeStruct
        return pl.pallas_call(
            functools.partial(gather_kernel, chips),
            name="gather",
            out_shape=(
                shape((tokens, depth), BF16),
                shape((tokens, depth), BF16),
                shape((tokens, cols), BF16),
                shape((rows, depth), F32),
                shape((early, depth), BF16),
                shape((LATE, depth), BF16),
                shape((early, depth), BF16),
                shape((LATE, depth), BF16),
                shape((EDGE, depth), BF16),
                shape((EDGE, depth), BF16),
                shape((cols, depth), BF16),
            ),
            in_specs=[anywhere] * 5,
            out_specs=(anywhere,) * 11,
            scratch_shapes=[
                pltpu.VMEM((cols, depth), BF16),
                pltpu.VMEM((depth, cols), BF16),
                pltpu.VMEM((depth, cols), BF16),
                pltpu.VMEM((CORES * rows, depth), BF16),
                pltpu.VMEM((CORES * rows, cols), BF16),
                pltpu.VMEM((CORES * rows, cols), BF16),
                pltpu.VMEM((chips, rows, cols), BF16),
                pltpu.VMEM((rows, depth), F32),
                pltpu.VMEM((rows, depth), BF16),
                pltpu.VMEM((rows, depth), F32),
                pltpu.VMEM((rows, depth), BF16),
                pltpu.VMEM((2 * EDGE, depth), BF16),
                pltpu.VMEM((cols, depth), F32),
                pltpu.SemaphoreType.DMA((2, COPIES)),
                pltpu.SemaphoreType.DMA((2, COPIES)),
                pltpu.SemaphoreType.DMA,
                pltpu.SemaphoreType.DMA((chips,)),
                pltpu.SemaphoreType.DMA,
                pltpu.SemaphoreType.DMA,
                pltpu.SemaphoreType.DMA((5,)),
                pltpu.SemaphoreType.DMA((5,)),
                pltpu.SemaphoreType.DMA((2,)),
                pltpu.SemaphoreType.DMA((2,)),
                pltpu.SemaphoreType.DMA((4,)),
                pltpu.SemaphoreType.DMA((6,)),
            ],
            compiler_params=pltpu.CompilerParams(
                collective_id=0, has_side_effects=True, vmem_limit_bytes=64 * 1024 * 1024 - 65536
            ),
            cost_estimate=pl.CostEstimate(
                flops=6 * tokens * depth * cols, bytes_accessed=8 * tokens * depth, transcendentals=0
            ),
        )(x, dy, pre, w_in, w_down)

    def weight_grad(xg, d_pre, done, tile=384):
        tokens, depth = xg.shape
        cols = d_pre.shape[1]
        steps = depth // tile

        def body(x_ref, d_ref, done_ref, out_ref, copy_ref):
            copy_ref[...] = done_ref[...]
            out_ref[...] = lax.dot_general(x_ref[...], d_ref[...], TN, preferred_element_type=F32).astype(BF16)

        side = pl.BlockSpec((done.shape[0] // steps, done.shape[1]), lambda i: (i, 0))
        return pl.pallas_call(
            body, name="weight_grad", grid=(steps,),
            in_specs=[pl.BlockSpec((tokens, tile), lambda i: (0, i)), pl.BlockSpec((tokens, cols), lambda i: (0, 0)), side],
            out_specs=(pl.BlockSpec((tile, cols), lambda i: (i, 0)), side),
            out_shape=(jax.ShapeDtypeStruct((depth, cols), BF16), jax.ShapeDtypeStruct(done.shape, done.dtype)),
            compiler_params=pltpu.CompilerParams(vmem_limit_bytes=55 * 1024 * 1024),
            cost_estimate=pl.CostEstimate(
                flops=2 * tokens * depth * cols, bytes_accessed=2 * tokens * (depth + cols) + 6 * depth * cols, transcendentals=0
            ),
        )(xg, d_pre, done)

    def keep_in_hbm(a):
        anywhere = pl.BlockSpec(memory_space=pl.ANY)
        return pl.pallas_call(
            lambda a_ref, out_ref: None, name="keep_in_hbm", in_specs=[anywhere], out_specs=anywhere,
            out_shape=jax.ShapeDtypeStruct(a.shape, a.dtype), input_output_aliases={0: 0},
        )(a)

    def step(x, dy, pre, w_in, w_down):
        clockwise = [(i, (i + CORES) % n) for i in range(n)]
        counter = [(i, (i - CORES) % n) for i in range(n)]
        (
            xg, _, d_pre, s_own, go_left, go_left_late, go_right, go_right_late, got_left, got_right, dw_down
        ) = gather(x, dy, pre, w_in, w_down)
        from_left = lax.ppermute(go_right, "tp", clockwise)
        from_right = lax.ppermute(go_left, "tp", counter)
        from_left_late = lax.ppermute(go_right_late, "tp", clockwise)
        from_right_late = lax.ppermute(go_left_late, "tp", counter)
        dw_in, dw_down = weight_grad(xg, d_pre, dw_down)
        s_own, dw_in, dw_down = lax.optimization_barrier((s_own, dw_in, dw_down))
        mid = go_right.shape[0]
        lower, upper = from_left[EDGE:], from_right[:mid - EDGE]
        dx = jnp.concatenate([
            s_own[:EDGE] + from_left[:EDGE].astype(F32) + got_right.astype(F32),
            s_own[EDGE:mid] + lower.astype(F32) + upper.astype(F32),
            jnp.zeros_like(s_own[:LATE]),
            s_own[mid + LATE:] + got_left.astype(F32) + from_right[mid - EDGE:].astype(F32),
        ]).astype(BF16)
        dx = keep_in_hbm(dx)
        late = s_own[mid:mid + LATE] + from_left_late.astype(F32) + from_right_late.astype(F32)
        dx = lax.dynamic_update_slice(dx, late.astype(BF16), (mid, 0))
        return dx, dw_in, dw_down

    tokens, columns, weight_rows = P(("dp", "tp"), None), P(None, "tp"), P("tp", None)
    return jax.shard_map(
        step,
        mesh=mesh,
        in_specs=(tokens, tokens, P("dp", "tp"), columns, weight_rows),
        out_specs=(tokens, P("dp", "tp"), P(("dp", "tp"), None)),
        check_vma=False,
    )
```
